512 devices in a mesh: row: 32 (over y, x), col: 16 (over z, core).
Axes of the slice: x: 4, y: 8, z: 8, core: 2. Of those that a mesh axis runs over, the one named last changes fastest.
Arguments:
- tokens: bfloat16 [24576, 2048], P('row', 'col'), may hold values from -6 to 6
- out_grad: bfloat16 [24576, 2048], P('row', 'col'), may hold values from -3072 to 3072
- counts: int32 [32], P('row'), may hold values from 65 to 768
- block_moves: int32 [16, 3], replicated, may hold values from 0 to 31, as said below
- segment_ids: int32 [24576], P('row'), may hold values from 0 to 767, never falling along the last dimension, each value on 1 to 128 neighbouring positions
- gate_weight: bfloat16 [2048, 8192], P('row', 'col'), may hold values from -0.125 to 0.125
- up_weight: bfloat16 [2048, 8192], P('row', 'col'), may hold values from -0.125 to 0.125
- down_weight: bfloat16 [2048, 8192], P('row', 'col'), may hold values from -0.0625 to 0.0625
Outputs:
- hidden: bfloat16 [16384, 8192], P('row', 'col')
- gate_grad: float32 [2048, 8192], P('row', 'col')
- up_grad: float32 [2048, 8192], P('row', 'col')
- down_grad: float32 [2048, 8192], P('row', 'col')
The draws below stay inside these ranges and needn't reach their ends.
Inputs may be any that keep to these rules, and one draw needn't show every extreme that they name: `block_moves`: each row is (source rank, destination rank, block index); the block is a valid block of its source; no two rows share both source and destination, nor both source and block; a rank is the source of at most two rows or the destination of at most one, never both; after the moves every rank holds at most 4 valid blocks and some hold exactly 4. `segment_ids`: never falling along the whole array; each document covers 1 to 128 consecutive slots.
All inputs are finite; a program needn't handle non-finite values.
Results may differ from the reference program's by a relative error of at most 0.015.
Values may be sent and summed in bfloat16 or wider, within the bound.
A program may use at most 64 MiB of HBM per device.

```python
import math
import jax
import jax.numpy as jnp
import numpy as np
from jax import lax

D = 2048
F = 8192
BLOCK = 128
WORK = 4
CAP = 6
TOK_DEV = 768
TOKENS = 24576
MOVES = 16
N_ROW = 32


def rebalance_plan(key):
    perm_key, light_key, part_key, pick_key, flip_key = jax.random.split(key, 5)
    groups = N_ROW // 4
    half = N_ROW // 2
    pair_order = jax.random.permutation(perm_key, half).astype(jnp.int32).reshape(groups, 2)
    flips = jax.random.randint(flip_key, (groups, 2), 0, 2, dtype=jnp.int32)
    low_rank = pair_order
    high_rank = pair_order + half
    first_rank = jnp.where(flips == 0, low_rank, high_rank)
    second_rank = jnp.where(flips == 0, high_rank, low_rank)
    order_ranks = jnp.stack([first_rank[:, 0], second_rank[:, 0], first_rank[:, 1], second_rank[:, 1]], axis=1).astype(jnp.int32)
    spare_load = jax.random.randint(light_key, (groups,), 1, WORK + 1, dtype=jnp.int32)
    heavy_load = jnp.full((groups,), WORK + 2, jnp.int32)
    lean_load = jnp.full((groups,), WORK - 1, jnp.int32)
    all_loads = jnp.stack([heavy_load, lean_load, lean_load, spare_load], axis=1).reshape(-1)
    block_counts = jnp.zeros((N_ROW,), jnp.int32).at[order_ranks.reshape(-1)].set(all_loads)
    tail_fill = jax.random.randint(part_key, (N_ROW,), BLOCK // 2 + 1, BLOCK + 1, dtype=jnp.int32)
    counts = ((block_counts - 1) * BLOCK + tail_fill).astype(jnp.int32)
    chosen = jax.vmap(lambda sub_key: jax.random.permutation(sub_key, WORK + 2)[:2])(jax.random.split(pick_key, groups)).astype(jnp.int32)
    first_move = jnp.stack([order_ranks[:, 0], order_ranks[:, 1], chosen[:, 0]], axis=1)
    second_move = jnp.stack([order_ranks[:, 0], order_ranks[:, 2], chosen[:, 1]], axis=1)
    block_moves = jnp.stack([first_move, second_move], axis=1).reshape(N_ROW // 2, 3).astype(jnp.int32)
    return (counts, block_moves)


def draw_counts(key, part):
    return rebalance_plan(jax.random.fold_in(key, 11))[0]


def draw_block_moves(key, part):
    return rebalance_plan(jax.random.fold_in(key, 11))[1]


def level_of(key, extent, cuts, smallest, largest):
    loudness, own = 1.0, jax.random.fold_in(key, 6)
    for dim, shards_of in cuts:
        steps = jnp.exp(jax.random.uniform(jax.random.fold_in(own, dim), (shards_of,), jnp.float32, smallest / len(cuts), largest / len(cuts)))
        loudness = loudness * jnp.repeat(steps, extent[dim] // shards_of).reshape([-1 if axis == dim else 1 for axis in range(len(extent))])
    return loudness


def length_profile(number_of, total, reach, slope):
    loads = [(1 << 20) // math.isqrt(rank ** slope) + 1 for rank in range(2, number_of + 1)]
    surplus, given = total - reach - (number_of - 1), [1] * (number_of - 1)
    while surplus > 0:
        candidates = [i for i in range(number_of - 1) if given[i] < reach]
        mass, left = sum([loads[i] for i in candidates]), surplus
        for i in candidates:
            extra = min(reach - given[i], max(1, left * loads[i] // mass), surplus)
            given[i] = given[i] + extra
            surplus = surplus - extra
    return np.array([reach] + given)


def uneven_parts(rng, number_of, total, most, lean):
    if number_of == 2:
        one = jax.random.randint(rng, (), max(1, total - most), min(most, total - 1) + 1)
        return jnp.stack([one, total - one])
    sizes = jnp.asarray(length_profile(number_of, total, most, lean), jnp.int32)
    twos = (number_of - 1) // 2
    source_of, sink = sizes[1:1 + 2 * twos:2], sizes[2:2 + 2 * twos:2]
    slack = jnp.minimum(source_of - 1, most - sink)
    passed = jax.random.randint(jax.random.fold_in(rng, 1), (twos,), 0, 1 << 20) % (slack + 1)
    sizes = sizes.at[1:1 + 2 * twos:2].set(source_of - passed).at[2:2 + 2 * twos:2].set(sink + passed)
    return sizes[jax.random.permutation(jax.random.fold_in(rng, 2), number_of)]


def scatter_about(rng, extent, spread, limit, cuts=(), held_as=jnp.bfloat16):
    result = jax.random.normal(rng, extent, jnp.float32) * spread
    if len(cuts) > 0:
        result = level_of(rng, extent, cuts, -0.22, 0.18) * result
    return jnp.clip(result, min=-limit, max=limit).astype(held_as)


def setup_inputs(seed: int = 0) -> dict:
    splits = jax.random.split(jax.random.key(seed), 9)
    return {
        "tokens": scatter_about(splits[0], (TOKENS, D), 1.0, 6.0, ((0, 32), (1, 16))),
        "out_grad": scatter_about(splits[1], (TOKENS, D), (16 * N_ROW), 3072.0, ((0, 32), (1, 16))),
        "counts": draw_counts(jax.random.fold_in(splits[8], 71), 0),
        "block_moves": draw_block_moves(jax.random.fold_in(splits[8], 71), 0),
        "segment_ids": jnp.searchsorted(jnp.cumsum(uneven_parts(splits[4], TOKENS // 32, TOKENS, 128, 2)), jnp.arange(TOKENS), side="right").astype(jnp.int32),
        "gate_weight": scatter_about(splits[5], (D, F), D ** -0.5, 0.125, ((0, 32), (1, 16))),
        "up_weight": scatter_about(splits[6], (D, F), D ** -0.5, 0.125, ((0, 32), (1, 16))),
        "down_weight": scatter_about(splits[7], (D, F), F ** -0.5, 0.0625, ((0, 32), (1, 16))),
    }


def loss_mask(counts, segment_ids):
    segments = segment_ids.reshape(N_ROW, TOK_DEV)
    following = jnp.concatenate([segments[:, 1:], segments[:, -1:]], axis=1)
    places = jnp.arange(TOK_DEV, dtype=jnp.int32)[None, :]
    kept_flag = (places + 1 < counts[:, None]) & (following == segments)
    return kept_flag.astype(jnp.float32)


def work_index(counts, block_moves):
    source = block_moves[:, 0]
    target = block_moves[:, 1]
    block_id = block_moves[:, 2]
    rank_ids = jnp.arange(N_ROW, dtype=jnp.int32)
    block_ids = jnp.arange(CAP, dtype=jnp.int32)
    filled = (counts + BLOCK - 1) // BLOCK
    moved_out = jnp.any((source[None, None, :] == rank_ids[:, None, None]) & (block_id[None, None, :] == block_ids[None, :, None]), axis=2)
    kept_flag = (block_ids[None, :] < filled[:, None]) & jnp.logical_not(moved_out)
    arrive = target[None, :] == rank_ids[:, None]
    flag_bits = jnp.concatenate([kept_flag, arrive], axis=1).astype(jnp.int32)
    own_ids = (rank_ids[:, None] * CAP + block_ids[None, :]).astype(jnp.int32)
    came_ids = jnp.broadcast_to((source * CAP + block_id)[None, :], (N_ROW, MOVES)).astype(jnp.int32)
    source_ids = jnp.concatenate([own_ids, came_ids], axis=1)
    list_place = (jnp.cumsum(flag_bits, axis=1) - 1).astype(jnp.int32)
    slot_ids = jnp.arange(WORK, dtype=jnp.int32)
    slot_hit = (flag_bits[:, :, None] == 1) & (list_place[:, :, None] == slot_ids[None, None, :])
    chosen = jnp.sum(jnp.where(slot_hit, source_ids[:, :, None] + 1, 0), axis=1).astype(jnp.int32)
    return (chosen - 1).astype(jnp.int32)


def pick_blocks(block_rows, slot_index):
    flat_index = slot_index.reshape(-1)
    picked = jnp.take(block_rows, jnp.maximum(flat_index, 0), axis=0)
    live_rows = (flat_index >= 0).reshape((-1,) + (1,) * (picked.ndim - 1))
    return jnp.where(live_rows, picked, jnp.zeros_like(picked))


def local_terms(gate_sum, up_sum, back_sum):
    logistic = jax.nn.sigmoid(gate_sum)
    activated = gate_sum * logistic
    hidden = (activated * up_sum).astype(jnp.bfloat16)
    gate_back = (back_sum * up_sum * logistic * (1.0 + gate_sum * (1.0 - logistic))).astype(jnp.bfloat16)
    up_back = (back_sum * activated).astype(jnp.bfloat16)
    return hidden, gate_back, up_back


def contract(left_side, right_side):
    return lax.dot_general(left_side, right_side, (((0,), (0,)), ((), ())), preferred_element_type=jnp.float32)


def reference(tokens, out_grad, counts, block_moves, segment_ids, gate_weight, up_weight, down_weight):
    weight_mask = loss_mask(counts, segment_ids)
    loss_total = jnp.sum(weight_mask)
    slot_index = work_index(counts, block_moves)
    work_tokens = pick_blocks(tokens.reshape(N_ROW * CAP, BLOCK, D), slot_index).reshape(N_ROW, WORK * BLOCK, D)
    work_grad = pick_blocks(out_grad.reshape(N_ROW * CAP, BLOCK, D), slot_index).reshape(N_ROW, WORK * BLOCK, D)
    work_weight = pick_blocks(weight_mask.reshape(N_ROW * CAP, BLOCK), slot_index).reshape(N_ROW, WORK * BLOCK)

    def per_rank(running, inputs):
        tok_rows, grad_rows, row_weight = inputs
        gate_sum = jnp.dot(tok_rows, gate_weight, preferred_element_type=jnp.float32)
        up_sum = jnp.dot(tok_rows, up_weight, preferred_element_type=jnp.float32)
        back_sum = jnp.dot(grad_rows, down_weight, preferred_element_type=jnp.float32) * row_weight[:, None]
        hidden, gate_back, up_back = local_terms(gate_sum, up_sum, back_sum)
        weighted = grad_rows * row_weight.astype(jnp.bfloat16)[:, None]
        new_terms = (contract(tok_rows, gate_back), contract(tok_rows, up_back), contract(weighted, hidden))
        rounded = tuple(lax.optimization_barrier((term_sum / loss_total).astype(jnp.bfloat16)).astype(jnp.float32) for term_sum in new_terms)
        return tuple(total_part + new_part for total_part, new_part in zip(running, rounded)), hidden

    zero_sums = jnp.zeros((D, F), jnp.float32)
    grad_sums, hidden_all = lax.scan(per_rank, (zero_sums, zero_sums, zero_sums), (work_tokens, work_grad, work_weight))
    return hidden_all.reshape(N_ROW * WORK * BLOCK, F), grad_sums[0], grad_sums[1], grad_sums[2]
```

```python
import jax
import jax.numpy as jnp
from jax import lax
from jax.experimental import pallas as pl
from jax.experimental.pallas import tpu as pltpu
from jax.sharding import Mesh
from jax.sharding import PartitionSpec as P

BLOCK = 128
WORK = 4
CAP = 6
MOVES = 16
NX, NY, NZ = 4, 8, 8
ROWS = 64
HID = 512
COLS = 3 * HID
MAIN = 384
MSG = 4 * BLOCK + 16
YMSG = 2 * BLOCK + 16
MESH = pl.DeviceIdType.MESH
BF16, F32 = jnp.bfloat16, jnp.float32


def pick_kernel(counts, moves, loss, tok, grad, own, outbox, scal):
    y, x = lax.axis_index("y"), lax.axis_index("x")
    me = y * NX + x
    count = counts[0]
    zero, one = jnp.int32(0), jnp.int32(1)
    src = [moves[m, 0] for m in range(MOVES)]
    dst = [moves[m, 1] for m in range(MOVES)]
    blk = [moves[m, 2] for m in range(MOVES)]

    kept = zero
    chosen = [-one] * WORK
    for b in range(CAP):
        moved = zero
        for m in range(MOVES):
            moved = moved | jnp.where((src[m] == me) & (blk[m] == b), one, zero)
        stays = (b * BLOCK < count) & (moved == 0)
        for s in range(WORK):
            chosen[s] = jnp.where(stays & (kept == s), jnp.int32(b), chosen[s])
        kept = kept + jnp.where(stays, one, zero)

    left = zero
    leaving = [-one] * 2
    arrives = zero
    for m in range(MOVES):
        mine = src[m] == me
        for j in range(2):
            leaving[j] = jnp.where(mine & (left == j), blk[m], leaving[j])
        left = left + jnp.where(mine, one, zero)
        arrives = arrives | jnp.where(dst[m] == me, one, zero)

    def fetch(ref, index):
        at = pl.multiple_of(jnp.maximum(index, 0) * BLOCK, BLOCK)
        live = jnp.where(index >= 0, 1.0, 0.0).astype(F32)
        return (ref[pl.ds(at, BLOCK), :].astype(F32) * live).astype(BF16)

    for s in range(WORK):
        own[0, pl.ds(s * BLOCK, BLOCK), :] = fetch(tok, chosen[s])
        own[1, pl.ds(s * BLOCK, BLOCK), :] = fetch(grad, chosen[s])
    for j in range(2):
        outbox[pl.ds(2 * j * BLOCK, BLOCK), :] = fetch(tok, leaving[j])
        outbox[pl.ds((2 * j + 1) * BLOCK, BLOCK), :] = fetch(grad, leaving[j])
    total = loss[0]
    row = lax.broadcasted_iota(jnp.int32, (16, BLOCK), 0)
    parts = jnp.where(row == 2 * x, total // 256, jnp.where(row == 2 * x + 1, total % 256, 0))
    outbox[pl.ds(4 * BLOCK, 16), :] = parts.astype(F32).astype(BF16)

    nth = [zero] * MOVES
    for m in range(MOVES):
        for before in range(m):
            nth[m] = nth[m] + jnp.where(src[before] == src[m], one, zero)
    for d in range(NY):
        at = -one
        for m in range(MOVES):
            hit = (src[m] // NX == y) & (dst[m] == d * NX + x)
            at = jnp.where(hit, (src[m] % NX) * 2 + nth[m], at)
        for i in range(2 * NX):
            scal[d * 2 * NX + i] = jnp.where(at == i, 1.0, 0.0).astype(F32)
    for s in range(WORK):
        scal[2 * NX * NY + s] = jnp.where((arrives == 1) & (kept == s), 1.0, 0.0).astype(F32)


def pick(counts, moves, loss, tok, grad):
    vmem, smem = pl.BlockSpec(memory_space=pltpu.VMEM), pl.BlockSpec(memory_space=pltpu.SMEM)
    return pl.pallas_call(
        pick_kernel,
        out_shape=(
            jax.ShapeDtypeStruct((2, WORK * BLOCK, BLOCK), BF16),
            jax.ShapeDtypeStruct((MSG, BLOCK), BF16),
            jax.ShapeDtypeStruct((128,), F32),
        ),
        in_specs=[smem, smem, smem, vmem, vmem],
        out_specs=(vmem, vmem, smem),
    )(counts, moves, loss, tok, grad)


LENGTH = []


class Graph:
    def __init__(self):
        self.nodes = {}

    def send(self, name, link, size, needs, make):
        self.nodes[name] = ("send", link, size, tuple(needs), make)

    def work(self, name, cost, rank, needs, run):
        self.nodes[name] = ("work", cost, rank, tuple(needs), run)

    def order(self):
        rate, lag = 46.6e3, 2.4
        todo = list(self.nodes)
        done, flying, free, now, steps = set(), [], {}, 0.0, []
        while todo or flying:
            for name in [n for n in todo if self.nodes[n][0] == "send"]:
                _, link, size, needs, _ = self.nodes[name]
                if all(n in done for n in needs):
                    quick = link == "core"
                    begin = max(now, free.get(link, 0.0))
                    free[link] = begin + size / (rate * (12 if quick else 1))
                    flying.append((free[link] + (1.0 if quick else lag), len(steps), name))
                    steps.append(("start", name))
                    todo.remove(name)
            flying.sort()
            if flying and flying[0][0] <= now:
                name = flying.pop(0)[2]
                steps.append(("wait", name))
                done.add(name)
                continue
            ready = [
                (self.nodes[n][2], i, n)
                for i, n in enumerate(todo)
                if self.nodes[n][0] == "work" and all(m in done for m in self.nodes[n][3])
            ]
            if ready:
                name = min(ready)[2]
                steps.append(("run", name))
                now += self.nodes[name][1]
                done.add(name)
                todo.remove(name)
                continue
            if flying:
                now = flying[0][0]
        LENGTH.append(now)
        return steps


def big_kernel(scal, own, outbox, gate, up, down, hidden, gate_out, up_out, down_out,
               w, z, xt, acc, act, tb, slots, xbuf, ysend, yrecv, own3, send_sem, recv_sem, own_sem):
    y, x = lax.axis_index("y"), lax.axis_index("x")
    zz, core = lax.axis_index("z"), lax.axis_index("core")
    size_of = {"x": NX, "y": NY, "z": NZ}
    mine = {"x": x, "y": y, "z": zz}

    def step(axis, by):
        return lax.rem(mine[axis] + (by % size_of[axis]), size_of[axis])

    barrier = pltpu.get_barrier_semaphore()
    peers = [{"x": step("x", d)} for d in range(1, NX)] + [{"y": step("y", d)} for d in range(1, NY)]
    peers += [{"z": step("z", 1)}, {"z": step("z", -1)}, {"core": 1 - core}]
    for peer in peers:
        pl.semaphore_signal(barrier, inc=1, device_id=peer, device_id_type=MESH)

    own_rows = pl.ds(pl.multiple_of((y * NX + x) * ROWS, ROWS), ROWS)
    feature = zz * 2 + core
    local = [
        pltpu.make_async_copy(outbox, xbuf.at[pl.ds(pl.multiple_of(x * MSG, 16), MSG), :], own_sem.at[0]),
        pltpu.make_async_copy(gate, w.at[own_rows, pl.ds(0, HID)], own_sem.at[1]),
        pltpu.make_async_copy(up, w.at[own_rows, pl.ds(HID, HID)], own_sem.at[2]),
        pltpu.make_async_copy(down, w.at[own_rows, pl.ds(2 * HID, HID)], own_sem.at[3]),
        pltpu.make_async_copy(own.at[:, pl.ds(0, MAIN), :], z.at[feature, :, pl.ds(0, MAIN), :], own_sem.at[4]),
        pltpu.make_async_copy(own.at[:, pl.ds(MAIN, BLOCK), :], own3, own_sem.at[5]),
    ]
    for copy in local:
        copy.start()

    graph = Graph()
    index = {}

    def remote(name, link, size, needs, peer, views):
        i = index.setdefault(name, len(index))

        def make(receiver):
            source, target = views(receiver)
            return pltpu.make_async_remote_copy(
                src_ref=source, dst_ref=target, send_sem=send_sem.at[i], recv_sem=recv_sem.at[i],
                device_id=peer, device_id_type=MESH,
            )

        graph.send(name, link, size, needs, make)

    def spread(tag, axis, size, needs, piece):
        n = size_of[axis]
        arrived = {0: list(needs)}
        for hop in range(1, n // 2 + 1):
            for sign in (1, -1):
                part = None if hop < n // 2 else (0 if sign > 0 else 1)
                name = (tag, sign, hop)

                def views(receiver, sign=sign, hop=hop, part=part):
                    ref = piece(step(axis, -sign * (hop if receiver else hop - 1)), part, receiver)
                    return ref, ref

                remote(name, axis + "-+"[sign > 0], size if part is None else size // 2,
                       needs if hop == 1 else [(tag, sign, hop - 1)], {axis: step(axis, sign)}, views)
                arrived.setdefault((sign * hop) % n, []).append(name)
        return arrived

    def gather_sum(tag, axis, size, own_ready, piece, cost, finish):
        n = size_of[axis]
        slot = {}
        for hop in range(n // 2, 0, -1):
            for sign in (1, -1):
                name = (tag, sign, hop)
                part = None if hop < n // 2 else (0 if sign > 0 else 1)
                slot[sign, hop] = ref = slots.at[len(used)]
                used.append(name)
                if part is not None:
                    ref = ref.at[pl.ds(0, 16), :]

                def views(receiver, sign=sign, hop=hop, part=part, ref=ref):
                    return piece(step(axis, sign * hop), part), ref

                needs = own_ready(sign * hop % n) if hop == n // 2 else [("add", tag, sign, hop)]
                remote(name, axis + "-+"[sign > 0], size if part is None else size // 2, needs,
                       {axis: step(axis, sign)}, views)
                if hop > 1:

                    def add(sign=sign, hop=hop, part=part, ref=ref):
                        into = piece(step(axis, sign * (hop - 1)), part)
                        into[...] = (into[...].astype(F32) + ref[...].astype(F32)).astype(BF16)

                    graph.work(("add", tag, sign, hop - 1), cost, 0,
                               [name] + own_ready(sign * (hop - 1) % n), add)

        def fin():
            finish(piece(mine[axis], None), slot[1, 1], slot[-1, 1])

        graph.work(("fin", tag), 1.5 * cost, 0, [(tag, 1, 1), (tag, -1, 1)] + own_ready(0), fin)

    used = []

    for d in (1, 3, 2):
        def views(receiver, d=d):
            rows = pl.ds(pl.multiple_of((step("x", -d) if receiver else x) * MSG, 16), MSG)
            return xbuf.at[rows, :], xbuf.at[rows, :]
        remote(("mx", d), "x-" if d == 3 else "x+", MSG * BLOCK * 2 * (2 if d == 2 else 1), [],
               {"x": step("x", d)}, views)

    def select():
        counts_rows = sum(xbuf[pl.ds(i * MSG + 4 * BLOCK, 16), :].astype(F32) for i in range(NX)).astype(BF16)
        for d in range(NY):
            chosen = None
            for i in range(2 * NX):
                block = xbuf[pl.ds(i // 2 * MSG + i % 2 * 2 * BLOCK, 2 * BLOCK), :]
                term = block * scal[d * 2 * NX + i].astype(BF16)
                chosen = term if chosen is None else chosen + term
            ysend[d, pl.ds(0, 2 * BLOCK), :] = chosen
            ysend[d, pl.ds(2 * BLOCK, 16), :] = counts_rows

    graph.work("select", 0.8, 0, [("mx", d) for d in (1, 2, 3)], select)
    for d in (1, 7, 2, 6, 3, 5, 4):
        def views(receiver, d=d):
            if receiver:
                return ysend.at[y], yrecv.at[step("y", -d)]
            return ysend.at[step("y", d)], yrecv.at[y]
        remote(("my", d), "y-" if d > 4 else "y+", YMSG * BLOCK * 2 * min(d, 8 - d), ["select"],
               {"y": step("y", d)}, views)

    def merge():
        total = ysend[y].astype(F32)
        for d in range(1, NY):
            total = total + yrecv[step("y", d)].astype(F32)
        for t in range(2):
            z[feature, t, pl.ds(MAIN, BLOCK), :] = (
                total[t * BLOCK : (t + 1) * BLOCK] + own3[t].astype(F32)
            ).astype(BF16)

    graph.work("merge", 0.6, 0, [("my", d) for d in range(1, NY)], merge)

    def loss_total():
        counts_rows = ysend[y, pl.ds(2 * BLOCK, 16), :].astype(F32)
        for d in range(1, NY):
            counts_rows = counts_rows + yrecv[step("y", d), pl.ds(2 * BLOCK, 16), :].astype(F32)
        row = lax.broadcasted_iota(jnp.int32, (16, BLOCK), 0)
        parts = jnp.where(row % 2 == 0, 256.0 * counts_rows, counts_rows)
        return jnp.sum(parts, axis=0, keepdims=True)[:, 0:1]

    def shard(ref, at_y, at_x, base, part):
        first = pl.multiple_of((at_y * NX + at_x) * ROWS + base + (16 if part else 0), 16)
        return ref.at[pl.ds(first, 32 if part is None else 16), :]

    whole = 32 * COLS * 2
    ax = spread("ax", "x", whole, [], lambda o, part, r: shard(w, y, o, 0, part))
    by = spread("by", "y", whole, [], lambda o, part, r: shard(w, o, x, 32, part))
    ay, bx = {}, {}
    for e in ax:
        ay[e] = spread(("ay", e), "y", whole, ax[e], lambda o, part, r, e=e: shard(w, o, step("x", -e), 0, part))
    for f in by:
        bx[f] = spread(("bx", f), "x", whole, by[f], lambda o, part, r, f=f: shard(w, step("y", -f), o, 32, part))

    token_needs = []
    for tag, lo, rows, needs in (("zm", 0, MAIN, []), ("zl", MAIN, BLOCK, ["merge"])):
        def cut(at, part, lo=lo, rows=rows):
            if part is None:
                return z.at[at, :, pl.ds(lo, rows), :]
            return z.at[at, part, pl.ds(lo, rows), :]

        bytes_all = 2 * rows * BLOCK * 2
        arrived = spread(tag, "z", bytes_all, needs, lambda o, part, r, cut=cut: cut(o * 2 + core, part))
        for g, names in arrived.items():
            for i, name in enumerate(names if g else [None]):
                part = i if g == NZ // 2 else None

                def views(receiver, g=g, part=part, cut=cut):
                    ref = cut(step("z", -g) * 2 + (1 - core if receiver else core), part)
                    return ref, ref

                remote(("core", tag, g, i), "core", bytes_all if part is None else bytes_all // 2,
                       [name] if g else needs, {"core": 1 - core}, views)
                token_needs.append(("core", tag, g, i))
        token_needs += [name for names in arrived.values() for name in names]

    first = [True]

    def forward(f):
        start = first[0]
        first[0] = False
        at = step("y", -f)
        rows = pl.ds(pl.multiple_of(at * 256, 256), 256)
        for t, lo, hi in ((0, 0, 4), (1, 4, 6)):
            left = jnp.concatenate([z[at * 2, t], z[at * 2 + 1, t]], axis=1)

            def tile(n, _, left=left):
                cols = pl.ds(pl.multiple_of(n * 256, 256), 256)
                new = jnp.dot(left, w[rows, cols], preferred_element_type=F32)
                acc[:, cols] = new if start else acc[:, cols] + new
                return 0

            lax.fori_loop(lo, hi, tile, 0)

    for f in range(NY):
        needs = token_needs + [n for e in ay for n in ay[e][f]] + [n for e in bx[f] for n in bx[f][e]]
        graph.work(("fwd", f), 1.0, 2, needs, lambda f=f: forward(f))

    def turn(c):
        for t in range(2):
            xt[t, pl.ds(c * BLOCK, BLOCK), :] = z[c, t].T

    for c in range(2 * NZ):
        graph.work(("turn", c), 0.3, 3, token_needs, lambda c=c: turn(c))

    def pointwise():
        def rows_of(i, _):
            rows = pl.ds(pl.multiple_of(i * 64, 64), 64)
            g, u, b = acc[rows, 0:HID], acc[rows, HID : 2 * HID], acc[rows, 2 * HID : COLS]
            logistic = jax.nn.sigmoid(g)
            activated = g * logistic
            act[rows, 0:HID] = (b * u * logistic * (1.0 + g * (1.0 - logistic))).astype(BF16)
            act[rows, HID : 2 * HID] = (b * activated).astype(BF16)
            act[rows, 2 * HID : COLS] = (activated * u).astype(BF16)
            return 0

        lax.fori_loop(0, 8, rows_of, 0)

    graph.work("pointwise", 3.0, 2, [("fwd", f) for f in range(NY)] + [("turn", c) for c in range(2 * NZ)], pointwise)

    def store_hidden():
        last = act[pl.ds(MAIN, BLOCK), 2 * HID : COLS]
        stays = 1.0 - (scal[64] + scal[65] + scal[66])
        for s in range(WORK - 1):
            at = pl.ds(s * BLOCK, BLOCK)
            hidden[at, :] = act[at, 2 * HID : COLS] + last * scal[64 + s].astype(BF16)
        hidden[pl.ds(MAIN, BLOCK), :] = last * stays.astype(BF16)

    graph.work("hidden", 0.5, 9, ["pointwise"], store_hidden)

    def backward(j):
        rows = pl.ds(pl.multiple_of(step("y", j) * 256, 256), 256)
        for t, lo, hi in ((0, 0, 4), (1, 4, 6)):
            def tile(n, _, t=t):
                cols = pl.ds(pl.multiple_of(n * 256, 256), 256)
                tb[rows, cols] = jnp.dot(xt[t, rows, :], act[:, cols], preferred_element_type=F32).astype(BF16)
                return 0

            lax.fori_loop(lo, hi, tile, 0)

    for i, j in enumerate((4, 5, 3, 6, 2, 7, 1, 0)):
        graph.work(("bwd", j), 1.0, 1 + i, ["pointwise"], lambda j=j: backward(j))

    def plain(own_ref, one, other):
        own_ref[...] = (own_ref[...].astype(F32) + one[...].astype(F32) + other[...].astype(F32)).astype(BF16)

    def final(base):
        def run(own_ref, one, other):
            total = loss_total()
            for i, out in enumerate((gate_out, up_out, down_out)):
                cols = pl.ds(i * HID, HID)
                sums = own_ref[:, cols].astype(F32) + one[:, cols].astype(F32) + other[:, cols].astype(F32)
                out[pl.ds(base, 32), :] = sums / total
        return run

    for e in range(NX):
        gather_sum(("say", e), "y", whole, lambda j: [("bwd", j)],
                   lambda o, part, e=e: shard(tb, o, step("x", e), 0, part), 0.15, plain)
    for f in (4, 5, 3, 6, 2, 7, 1, 0):
        gather_sum(("sbx", f), "x", whole, lambda j, f=f: [("bwd", f)],
                   lambda o, part, f=f: shard(tb, step("y", f), o, 32, part), 0.15, plain)
    gather_sum("sax", "x", whole, lambda j: [("fin", ("say", j))],
               lambda o, part: shard(tb, y, o, 0, part), 0.15, final(0))
    gather_sum("sby", "y", whole, lambda j: [("fin", ("sbx", j))],
               lambda o, part: shard(tb, o, x, 32, part), 0.15, final(32))

    pl.semaphore_wait(barrier, len(peers))
    for copy in local:
        copy.wait()
    copies = {}
    for kind, name in graph.order():
        if kind == "run":
            graph.nodes[name][4]()
        elif kind == "start":
            copies[name] = graph.nodes[name][4](False)
            copies[name].start()
        else:
            graph.nodes[name][4](True).wait_recv()
    for copy in copies.values():
        copy.wait_send()


SLOTS = 76
SENDS = 206


def big(scal, own, outbox, gate, up, down):
    vmem, smem = pl.BlockSpec(memory_space=pltpu.VMEM), pl.BlockSpec(memory_space=pltpu.SMEM)
    anyw = pl.BlockSpec(memory_space=pl.ANY)
    grad = jax.ShapeDtypeStruct((ROWS, HID), F32)
    rows = WORK * BLOCK
    return pl.pallas_call(
        big_kernel,
        out_shape=(jax.ShapeDtypeStruct((rows, HID), BF16), grad, grad, grad),
        in_specs=[smem] + [anyw] * 5,
        out_specs=(vmem,) * 4,
        scratch_shapes=[
            pltpu.VMEM((NX * NY * ROWS, COLS), BF16),
            pltpu.VMEM((2 * NZ, 2, rows, BLOCK), BF16),
            pltpu.VMEM((2, 2 * NZ * BLOCK, rows), BF16),
            pltpu.VMEM((rows, COLS), F32),
            pltpu.VMEM((rows, COLS), BF16),
            pltpu.VMEM((NX * NY * ROWS, COLS), BF16),
            pltpu.VMEM((SLOTS, 32, COLS), BF16),
            pltpu.VMEM((NX * MSG, BLOCK), BF16),
            pltpu.VMEM((NY, YMSG, BLOCK), BF16),
            pltpu.VMEM((NY, YMSG, BLOCK), BF16),
            pltpu.VMEM((2, BLOCK, BLOCK), BF16),
            pltpu.SemaphoreType.DMA((SENDS,)),
            pltpu.SemaphoreType.DMA((SENDS,)),
            pltpu.SemaphoreType.DMA((6,)),
        ],
        compiler_params=pltpu.CompilerParams(
            collective_id=0, has_side_effects=True, vmem_limit_bytes=60 * 1024 * 1024
        ),
    )(scal, own, outbox, gate, up, down)


def on_device(tokens, out_grad, counts, block_moves, segment_ids, gate, up, down):
    places = jnp.arange(tokens.shape[0], dtype=jnp.int32)
    following = jnp.concatenate([segment_ids[1:], segment_ids[-1:]])
    keep = (places + 1 < counts[0]) & (following == segment_ids)
    loss = jnp.sum(keep.astype(jnp.int32)).reshape(1)
    weighted = out_grad * keep.astype(BF16)[:, None]
    own, outbox, scal = pick(counts, block_moves, loss, tokens, weighted)
    return big(scal, own, outbox, gate, up, down)


def solution(mesh):
    torus = Mesh(mesh.devices.reshape(NY, NX, NZ, 2), ("y", "x", "z", "core"))
    row, col = ("y", "x"), ("z", "core")
    return jax.shard_map(
        on_device,
        mesh=torus,
        in_specs=(P(row, col), P(row, col), P(row), P(), P(row), P(row, col), P(row, col), P(row, col)),
        out_specs=(P(row, col),) * 4,
        check_vma=False,
    )
```

```python
import jax
import jax.numpy as jnp
from jax import lax
from jax.experimental import pallas as pl
from jax.experimental.pallas import tpu as pltpu
from jax.sharding import Mesh
from jax.sharding import PartitionSpec as P

BLOCK = 128
WORK = 4
CAP = 6
MOVES = 16
NX, NY, NZ = 4, 8, 8
ROWS = 64
HID = 512
COLS = 3 * HID
MAIN = 384
MSG = 4 * BLOCK + 16
YMSG = 2 * BLOCK + 16
CUT = {"a": (0, 640), "b": (640, 896)}
MESH = pl.DeviceIdType.MESH
BF16, F32 = jnp.bfloat16, jnp.float32


def choose(y, x, counts, moves):
    me = y * NX + x
    count = counts[0]
    zero, one = jnp.int32(0), jnp.int32(1)
    src = [moves[0, m] for m in range(MOVES)]
    dst = [moves[1, m] for m in range(MOVES)]
    blk = [moves[2, m] for m in range(MOVES)]
    src_y = [lax.div(v, jnp.int32(NX)) for v in src]
    src_x = [v - NX * w for v, w in zip(src, src_y)]

    def factor(flag):
        return jnp.where(flag, 1.0, 0.0).astype(F32)

    left = zero
    leaving = [-one] * 2
    arrives = zero
    for m in range(MOVES):
        mine = src[m] == me
        for j in range(2):
            leaving[j] = jnp.where(mine & (left == j), blk[m], leaving[j])
        left = left + jnp.where(mine, one, zero)
        arrives = arrives | jnp.where(dst[m] == me, one, zero)
    kept = zero
    chosen = [-one] * WORK
    for b in range(CAP):
        stays = (b * BLOCK < count) & (leaving[0] != b) & (leaving[1] != b)
        for s in range(WORK):
            chosen[s] = jnp.where(stays & (kept == s), jnp.int32(b), chosen[s])
        kept = kept + jnp.where(stays, one, zero)
    stay = [[factor(chosen[s] == b) for b in range(CAP)] for s in range(WORK)]
    leave = [[factor(leaving[j] == b) for b in range(CAP)] for j in range(2)]

    second = [zero] * MOVES
    for m in range(MOVES):
        for before in range(m):
            second[m] = second[m] | jnp.where(src[before] == src[m], one, zero)
    route = []
    for d in range(NY):
        at = -one
        for m in range(MOVES):
            hit = (src_y[m] == y) & (dst[m] == d * NX + x)
            at = jnp.where(hit, src_x[m] * 2 + second[m], at)
        route.append([factor(at == i) for i in range(2 * NX)])
    slot = [factor((arrives == 1) & (kept == s)) for s in range(WORK)]
    return stay, leave, route, slot


def blend(factors, blocks):
    total = None
    for f, block in zip(factors, blocks):
        term = block * f.astype(BF16)
        total = term if total is None else total + term
    return total


TIMES = {}


class Graph:
    def __init__(self):
        self.nodes = {}

    def send(self, name, link, size, needs, make):
        self.nodes[name] = ("send", link, size, tuple(needs), make)

    def work(self, name, cost, rank, needs, run):
        self.nodes[name] = ("work", cost, rank, tuple(needs), run)

    def order(self):
        rate, lag = 46.6e3, 2.2
        nodes = self.nodes
        after = {n: [] for n in nodes}
        for n, node in nodes.items():
            for m in node[3]:
                after[m].append(n)
        below = {}

        def span(n):
            if nodes[n][0] == "work":
                return nodes[n][1]
            quick = nodes[n][1] == "core"
            return nodes[n][2] / (rate * (12 if quick else 1)) + (1.0 if quick else lag)

        def urgency(n):
            if n not in below:
                below[n] = span(n) + max([urgency(m) for m in after[n]], default=0.0)
            return below[n]

        todo = sorted(nodes, key=lambda n: -urgency(n))
        done, flying, free, now, steps = set(), [], {}, 0.0, []
        while todo or flying:
            ahead = 2.5 if ("fin", "my") in done else 0.6
            for name in [n for n in todo if nodes[n][0] == "send"]:
                _, link, size, needs, _ = nodes[name]
                quick = link == "core"
                if all(n in done for n in needs) and free.get(link, 0.0) - now < ahead:
                    begin = max(now, free.get(link, 0.0))
                    free[link] = begin + size / (rate * (12 if quick else 1))
                    flying.append((free[link] + (1.0 if quick else lag), len(steps), name))
                    steps.append(("start", name))
                    todo.remove(name)
            flying.sort()
            if flying and flying[0][0] <= now:
                name = flying.pop(0)[2]
                steps.append(("wait", name))
                done.add(name)
                continue
            ready = [n for n in todo if nodes[n][0] == "work" and all(m in done for m in nodes[n][3])]
            if ready:
                steps.append(("run", ready[0]))
                now += nodes[ready[0]][1]
                TIMES[ready[0]] = now
                done.add(ready[0])
                todo.remove(ready[0])
                continue
            if flying:
                now = flying[0][0]
        TIMES["end"] = now
        return steps


def big_kernel(counts, moves, seg, tok, grad, gate, up, down, hidden_out, sums_hbm,
               w, z, xt, acc, act, tb, slots_a, slots_b, slots_m, xbuf, ysend, own3, tokv, gradv, marks, hidden, sums_out,
               send_sem, recv_sem, own_sem):
    y, x = lax.axis_index("y"), lax.axis_index("x")
    zz, core = lax.axis_index("z"), lax.axis_index("core")
    size_of = {"x": NX, "y": NY, "z": NZ}
    mine = {"x": x, "y": y, "z": zz}

    def step(axis, by):
        return lax.rem(mine[axis] + (by % size_of[axis]), size_of[axis])

    barrier = pltpu.get_barrier_semaphore()
    peers = [{axis: step(axis, by)} for axis in ("x", "y", "z") for by in (1, -1)] + [{"core": 1 - core}]
    for peer in peers:
        pl.semaphore_signal(barrier, inc=1, device_id=peer, device_id_type=MESH)

    own_rows = pl.ds(pl.multiple_of((y * NX + x) * ROWS, ROWS), ROWS)
    feature = zz * 2 + core
    local = [
        pltpu.make_async_copy(gate, w.at[own_rows, pl.ds(0, HID)], own_sem.at[0]),
        pltpu.make_async_copy(up, w.at[own_rows, pl.ds(HID, HID)], own_sem.at[1]),
        pltpu.make_async_copy(down, w.at[own_rows, pl.ds(2 * HID, HID)], own_sem.at[2]),
    ]
    local_rows = [
        pltpu.make_async_copy(tok, tokv, own_sem.at[3]),
        pltpu.make_async_copy(grad, gradv, own_sem.at[4]),
    ]
    for copy in local + local_rows:
        copy.start()
    stay, leave, route, slot_of = choose(y, x, counts, moves)

    graph = Graph()
    index = {}

    def remote(name, link, size, needs, peer, views):
        i = index.setdefault(name, len(index))

        def make(receiver):
            source, target = views(receiver)
            return pltpu.make_async_remote_copy(
                src_ref=source, dst_ref=target, send_sem=send_sem.at[i], recv_sem=recv_sem.at[i],
                device_id=peer, device_id_type=MESH,
            )

        graph.send(name, link, size, needs, make)

    def spread(tag, axis, size, needs, piece):
        n = size_of[axis]
        arrived = {0: list(needs)}
        for hop in range(1, n // 2 + 1):
            for sign in (1, -1):
                part = None if hop < n // 2 else (0 if sign > 0 else 1)
                name = (tag, sign, hop)

                def views(receiver, sign=sign, hop=hop, part=part):
                    ref = piece(step(axis, -sign * (hop if receiver else hop - 1)), part, receiver)
                    return ref, ref

                remote(name, axis + "-+"[sign > 0], size if part is None else size // 2,
                       needs if hop == 1 else [(tag, sign, hop - 1)], {axis: step(axis, sign)}, views)
                arrived.setdefault((sign * hop) % n, []).append(name)
        return arrived

    def gather_sum(tag, axis, size, own_ready, piece, cost, finish, pool, halves):
        n = size_of[axis]
        slot = {}
        slots, used = pool
        for hop in range(n // 2, 0, -1):
            for sign in (1, -1):
                name = (tag, sign, hop)
                part = None if hop < n // 2 else (0 if sign > 0 else 1)
                slot[sign, hop] = ref = slots.at[len(used)]
                used.append(name)
                if part is not None:
                    ref = ref.at[halves[part], :]

                def views(receiver, sign=sign, hop=hop, part=part, ref=ref):
                    return piece(step(axis, sign * hop), part), ref

                needs = own_ready(sign * hop % n) if hop == n // 2 else [("add", tag, sign, hop)]
                remote(name, axis + "-+"[sign > 0], size if part is None else size // 2, needs,
                       {axis: step(axis, sign)}, views)
                if hop > 1:

                    def add(sign=sign, hop=hop, part=part, ref=ref):
                        into = piece(step(axis, sign * (hop - 1)), part)
                        into[...] = (into[...].astype(F32) + ref[...].astype(F32)).astype(BF16)

                    graph.work(("add", tag, sign, hop - 1), cost, 0,
                               [name] + own_ready(sign * (hop - 1) % n), add)

        def fin():
            finish(piece(mine[axis], None), slot[1, 1], slot[-1, 1])

        graph.work(("fin", tag), 1.5 * cost, 0, [(tag, 1, 1), (tag, -1, 1)] + own_ready(0), fin)

    pool_a, pool_b, pool_m = (slots_a, []), (slots_b, []), (slots_m, [])

    def prepare():
        lane = lax.broadcasted_iota(jnp.int32, (8, BLOCK), 1)
        line = lax.broadcasted_iota(jnp.int32, (8, BLOCK), 0)
        now = jnp.concatenate([seg[...], seg[0:2, :]], axis=0)
        down_one = jnp.concatenate([now[1:8, :], now[0:1, :]], axis=0)
        after = jnp.where(lane == BLOCK - 1, down_one[:, 0:1], pltpu.roll(now, BLOCK - 1, 1))
        keep = jnp.where((line * BLOCK + lane + 1 < counts[0]) & (after == now), 1.0, 0.0).astype(F32)
        marks[...] = jnp.zeros_like(marks)
        marks[pl.ds(0, 8), :] = keep
        columns = marks[...].T
        for copy in local_rows:
            copy.wait()
        for b in range(CAP):
            at = pl.ds(b * BLOCK, BLOCK)
            gradv[at, :] = (gradv[at, :].astype(F32) * columns[:, b : b + 1]).astype(BF16)
        blocks = [pl.ds(b * BLOCK, BLOCK) for b in range(CAP)]
        first_row = pl.multiple_of(x * MSG, 16)
        for t, ref in enumerate((tokv, gradv)):
            for j in range(2):
                xbuf[pl.ds(first_row + (2 * j + t) * BLOCK, BLOCK), :] = blend(leave[j], [ref[at, :] for at in blocks])
        total = jnp.sum(jnp.sum(keep, axis=0, keepdims=True), axis=1, keepdims=True)
        high = jnp.floor(total * (1 / 256))
        middle = jnp.floor((total - 256.0 * high) * (1 / 16))
        low = total - 256.0 * high - 16.0 * middle
        row = lax.broadcasted_iota(jnp.int32, (16, BLOCK), 0) - 3 * x
        digits = jnp.where(row == 0, high, jnp.where(row == 1, middle, jnp.where(row == 2, low, 0.0)))
        xbuf[pl.ds(first_row + 4 * BLOCK, 16), :] = digits.astype(BF16)

    def prepare_own():
        blocks = [pl.ds(b * BLOCK, BLOCK) for b in range(CAP)]
        for t, ref in enumerate((tokv, gradv)):
            for s in range(WORK):
                rows = blend(stay[s][s:], [ref[at, :] for at in blocks[s:]])
                if s < WORK - 1:
                    z[feature, t, pl.ds(s * BLOCK, BLOCK), :] = rows
                else:
                    own3[t] = rows

    graph.work("own", 0.3, 0, [], prepare_own)

    def message(o, part):
        lo, n = (0, MSG) if part is None else ((0, 2 * BLOCK), (2 * BLOCK, MSG - 2 * BLOCK))[part]
        return xbuf.at[pl.ds(pl.multiple_of(o * MSG + lo, 16), n), :]

    mx = spread("mx", "x", MSG * BLOCK * 2, [], lambda o, part, r: message(o, part))

    def select():
        digits = sum(xbuf[pl.ds(i * MSG + 4 * BLOCK, 16), :].astype(F32) for i in range(NX)).astype(BF16)
        for d in range(NY):
            for t in range(2):
                blocks = [xbuf[pl.ds(i // 2 * MSG + (i % 2 * 2 + t) * BLOCK, BLOCK), :] for i in range(2 * NX)]
                ysend[d, pl.ds(t * BLOCK, BLOCK), :] = blend(route[d], blocks)
            ysend[d, pl.ds(2 * BLOCK, 16), :] = digits

    graph.work("select", 0.5, 0, [n for names in mx.values() for n in names], select)
    move_halves = (pl.ds(0, BLOCK), pl.ds(BLOCK, BLOCK + 16))

    def merge(own_ref, one, other):
        total = own_ref[...].astype(F32) + one[...].astype(F32) + other[...].astype(F32)
        for t in range(2):
            z[feature, t, pl.ds(MAIN, BLOCK), :] = (
                total[t * BLOCK : (t + 1) * BLOCK] + own3[t].astype(F32)
            ).astype(BF16)
        own_ref[...] = total.astype(BF16)

    gather_sum("my", "y", YMSG * BLOCK * 2, lambda j: ["select"],
               lambda o, part: ysend.at[o] if part is None else ysend.at[o, move_halves[part], :],
               0.15, merge, pool_m, move_halves)
    merged = ("fin", "my")

    def loss_total():
        digits = ysend[y, pl.ds(2 * BLOCK, 16), :].astype(F32)
        row = lax.broadcasted_iota(jnp.int32, (16, BLOCK), 0) % 3
        parts = jnp.where(row == 0, 256.0 * digits, jnp.where(row == 1, 16.0 * digits, digits))
        return jnp.sum(parts, axis=0, keepdims=True)[:, 0:1]

    row_halves = (pl.ds(0, 32), pl.ds(32, 32))

    def shard(ref, at_y, at_x, cut, part):
        first = pl.multiple_of((at_y * NX + at_x) * ROWS + (32 if part else 0), 32)
        return ref.at[pl.ds(first, ROWS if part is None else 32), pl.ds(*CUT[cut])]

    size_a, size_b = ROWS * CUT["a"][1] * 2, ROWS * CUT["b"][1] * 2
    by = spread("by", "y", size_b, [], lambda o, part, r: shard(w, o, x, "b", part))
    ax = spread("ax", "x", size_a, mx[1] + mx[3], lambda o, part, r: shard(w, y, o, "a", part))
    ay, bx = {}, {}
    for e in ax:
        ay[e] = spread(("ay", e), "y", size_a, ax[e], lambda o, part, r, e=e: shard(w, o, step("x", -e), "a", part))
    for f in by:
        bx[f] = spread(("bx", f), "x", size_b, by[f] or mx[1] + mx[3], lambda o, part, r, f=f: shard(w, step("y", -f), o, "b", part))

    have = {}
    for tag, lo, rows, needs, t in (
        ("zm", 0, MAIN, ["own"], None), ("zl0", MAIN, BLOCK, [merged], 0), ("zl1", MAIN, BLOCK, [merged], 1),
    ):
        def cut(at, part, lo=lo, rows=rows, t=t):
            if t is not None:
                lo, rows = (lo, rows) if part is None else (lo + part * (rows // 2), rows // 2)
                return z.at[at, t, pl.ds(lo, rows), :]
            if part is None:
                return z.at[at, :, pl.ds(lo, rows), :]
            return z.at[at, part, pl.ds(lo, rows), :]

        bytes_all = (2 if t is None else 1) * rows * BLOCK * 2
        arrived = spread(tag, "z", bytes_all, needs, lambda o, part, r, cut=cut: cut(o * 2 + core, part))
        for g, names in arrived.items():
            for i, name in enumerate(names if g else [None]):
                part = i if g == NZ // 2 else None

                def views(receiver, g=g, part=part, cut=cut):
                    ref = cut(step("z", -g) * 2 + (1 - core if receiver else core), part)
                    return ref, ref

                remote(("core", tag, g, i), "core", bytes_all if part is None else bytes_all // 2,
                       [name] if g else needs, {"core": 1 - core}, views)
                have.setdefault(tag[:2], []).append(("core", tag, g, i))
        have[tag[:2]] += [name for names in arrived.values() for name in names]

    seen = []

    def forward(f):
        start = not seen
        seen.append(f)
        at = step("y", -f)
        rows = pl.ds(pl.multiple_of(at * 256, 256), 256)
        slots = pl.ds(0, MAIN)
        for t, lo, hi in ((0, 0, 4), (1, 4, 6)):
            left = jnp.concatenate([z[at * 2, t, slots, :], z[at * 2 + 1, t, slots, :]], axis=1)

            def tile(n, _, left=left):
                cols = pl.ds(pl.multiple_of(n * 256, 256), 256)
                new = jnp.dot(left, w[rows, cols], preferred_element_type=F32)
                acc[slots, cols] = new if start else acc[slots, cols] + new
                return 0

            lax.fori_loop(lo, hi, tile, 0)

    def forward_last():
        slots = pl.ds(MAIN, BLOCK)
        for t, lo, hi in ((0, 0, 2), (1, 2, 3)):
            left = jnp.concatenate([z[c, t, slots, :] for c in range(2 * NZ)], axis=1)

            def tile(n, _, left=left):
                cols = pl.ds(pl.multiple_of(n * 512, 512), 512)
                acc[slots, cols] = jnp.dot(left, w[:, cols], preferred_element_type=F32)
                return 0

            lax.fori_loop(lo, hi, tile, 0)

    all_landed = []
    for f in range(NY):
        landed = [n for e in ay for n in ay[e][f]] + [n for e in bx[f] for n in bx[f][e]]
        all_landed += landed
        graph.work(("fwd", f), 1.3, 2, have["zm"] + landed, lambda f=f: forward(f))
    graph.work("fwd last", 2.5, 2, have["zl"] + all_landed, forward_last)
    parts_of = (("zm", 0, MAIN, 1.1), ("zl", MAIN, BLOCK, 0.5))

    def turn(c, lo, n_rows):
        for t in range(2):
            xt[t, pl.ds(c * BLOCK, BLOCK), pl.ds(lo, n_rows)] = z[c, t, pl.ds(lo, n_rows), :].T

    for tag, lo, n_rows, cost in parts_of:
        for c in range(2 * NZ):
            graph.work(("turn", tag, c), 0.2 * cost, 3, have[tag], lambda c=c, lo=lo, n_rows=n_rows: turn(c, lo, n_rows))

    def pointwise():
        def rows_of(i, _):
            rows = pl.ds(pl.multiple_of(i * 64, 64), 64)
            g, u, b = acc[rows, 0:HID], acc[rows, HID : 2 * HID], acc[rows, 2 * HID : COLS]
            logistic = jax.nn.sigmoid(g)
            activated = g * logistic
            act[rows, 0:HID] = (b * u * logistic * (1.0 + g * (1.0 - logistic))).astype(BF16)
            act[rows, HID : 2 * HID] = (b * activated).astype(BF16)
            act[rows, 2 * HID : COLS] = (activated * u).astype(BF16)
            return 0

        lax.fori_loop(0, 8, rows_of, 0)

    graph.work("pointwise", 0.6, 2, [("fwd", f) for f in range(NY)] + ["fwd last"]
               + [("turn", tag, c) for tag in have for c in range(2 * NZ)], pointwise)

    def store_hidden():
        last = act[pl.ds(MAIN, BLOCK), 2 * HID : COLS]
        for s in range(WORK - 1):
            at = pl.ds(s * BLOCK, BLOCK)
            hidden[at, :] = act[at, 2 * HID : COLS] + last * slot_of[s].astype(BF16)
        stays = 1.0 - (slot_of[0] + slot_of[1] + slot_of[2])
        hidden[pl.ds(MAIN, BLOCK), :] = last * stays.astype(BF16)

    hidden_copy = pltpu.make_async_copy(hidden, hidden_out, own_sem.at[5])
    sums_copy = pltpu.make_async_copy(sums_out, sums_hbm, own_sem.at[6])

    graph.work("hidden", 0.3, 9, [("bwd", 0)], store_hidden)
    graph.work("send hidden", 0.0, 9, [("fin", ("sbx", 0)), "hidden"], hidden_copy.start)

    def backward(j):
        rows = pl.ds(pl.multiple_of(step("y", j) * 256, 256), 256)
        for t, lo, hi in ((0, 0, 2), (1, 2, 3)):
            left = xt[t, rows, :]

            def tile(n, _, left=left):
                cols = pl.ds(pl.multiple_of(n * 512, 512), 512)
                tb[rows, cols] = jnp.dot(left, act[:, cols], preferred_element_type=F32).astype(BF16)
                return 0

            lax.fori_loop(lo, hi, tile, 0)

    for i, j in enumerate((4, 5, 3, 6, 2, 7, 1, 0)):
        graph.work(("bwd", j), 1.0, 1 + i, ["pointwise"], lambda j=j: backward(j))

    def plain(own_ref, one, other):
        own_ref[...] = (own_ref[...].astype(F32) + one[...].astype(F32) + other[...].astype(F32)).astype(BF16)

    def final(cut):
        def run(own_ref, one, other):
            sums = own_ref[...].astype(F32) + one[...].astype(F32) + other[...].astype(F32)
            sums_out[:, pl.ds(*CUT[cut])] = sums / loss_total()
        return run

    for e in (2, 1, 3, 0):
        gather_sum(("say", e), "y", size_a, lambda j: [("bwd", j)],
                   lambda o, part, e=e: shard(tb, o, step("x", e), "a", part), 0.15, plain, pool_a, row_halves)
    for f in (4, 5, 3, 6, 2, 7, 1, 0):
        gather_sum(("sbx", f), "x", size_b, lambda j, f=f: [("bwd", f)],
                   lambda o, part, f=f: shard(tb, step("y", f), o, "b", part), 0.15, plain, pool_b, row_halves)
    gather_sum("sax", "x", size_a, lambda j: [("fin", ("say", j))],
               lambda o, part: shard(tb, y, o, "a", part), 0.15, final("a"), pool_a, row_halves)
    gather_sum("sby", "y", size_b, lambda j: [("fin", ("sbx", j))],
               lambda o, part: shard(tb, o, x, "b", part), 0.15, final("b"), pool_b, row_halves)

    prepare()
    for copy in local:
        copy.wait()
    pl.semaphore_wait(barrier, len(peers))
    copies = {}
    for kind, name in graph.order():
        if kind == "run":
            graph.nodes[name][4]()
        elif kind == "start":
            copies[name] = graph.nodes[name][4](False)
            copies[name].start()
        else:
            graph.nodes[name][4](True).wait_recv()
    sums_copy.start()
    for copy in copies.values():
        copy.wait_send()
    hidden_copy.wait()
    sums_copy.wait()


SENDS = 240


def big(counts, moves, seg, tok, grad, gate, up, down):
    vmem, smem = pl.BlockSpec(memory_space=pltpu.VMEM), pl.BlockSpec(memory_space=pltpu.SMEM)
    anyw = pl.BlockSpec(memory_space=pl.ANY)
    rows = WORK * BLOCK
    return pl.pallas_call(
        big_kernel,
        out_shape=(jax.ShapeDtypeStruct((rows, HID), BF16), jax.ShapeDtypeStruct((ROWS, COLS), F32)),
        in_specs=[smem, smem, vmem] + [anyw] * 5,
        out_specs=(anyw,) * 2,
        scratch_shapes=[
            pltpu.VMEM((NX * NY * ROWS, COLS), BF16),
            pltpu.VMEM((2 * NZ, 2, rows, BLOCK), BF16),
            pltpu.VMEM((2, 2 * NZ * BLOCK, rows), BF16),
            pltpu.VMEM((rows, COLS), F32),
            pltpu.VMEM((rows, COLS), BF16),
            pltpu.VMEM((NX * NY * ROWS, COLS), BF16),
            pltpu.VMEM((36, ROWS, CUT["a"][1]), BF16),
            pltpu.VMEM((40, ROWS, CUT["b"][1]), BF16),
            pltpu.VMEM((8, YMSG, BLOCK), BF16),
            pltpu.VMEM((NX * MSG, BLOCK), BF16),
            pltpu.VMEM((NY, YMSG, BLOCK), BF16),
            pltpu.VMEM((2, BLOCK, BLOCK), BF16),
            pltpu.VMEM((CAP * BLOCK, BLOCK), BF16),
            pltpu.VMEM((CAP * BLOCK, BLOCK), BF16),
            pltpu.VMEM((BLOCK, BLOCK), F32),
            pltpu.VMEM((rows, HID), BF16),
            pltpu.VMEM((ROWS, COLS), F32),
            pltpu.SemaphoreType.DMA((SENDS,)),
            pltpu.SemaphoreType.DMA((SENDS,)),
            pltpu.SemaphoreType.DMA((7,)),
        ],
        compiler_params=pltpu.CompilerParams(
            collective_id=0, has_side_effects=True, vmem_limit_bytes=60 * 1024 * 1024
        ),
    )(counts, moves, seg, tok, grad, gate, up, down)


def finish_kernel(hidden_in, sums, hidden, gate_out, up_out, down_out):
    hidden[...] = hidden_in[...]
    for i, out in enumerate((gate_out, up_out, down_out)):
        out[...] = sums[:, i * HID : (i + 1) * HID]


def finish(hidden, sums):
    vmem = pl.BlockSpec(memory_space=pltpu.VMEM)
    grad = jax.ShapeDtypeStruct((ROWS, HID), F32)
    return pl.pallas_call(
        finish_kernel,
        out_shape=(jax.ShapeDtypeStruct(hidden.shape, BF16), grad, grad, grad),
        in_specs=[vmem, vmem],
        out_specs=(vmem,) * 4,
    )(hidden, sums)


def on_device(tokens, out_grad, counts, block_moves, segment_ids, gate, up, down):
    seg = segment_ids.reshape(CAP, BLOCK)
    hidden, sums = big(counts, block_moves.T, seg, tokens, out_grad, gate, up, down)
    return finish(hidden, sums)


def solution(mesh):
    torus = Mesh(mesh.devices.reshape(NY, NX, NZ, 2), ("y", "x", "z", "core"))
    row, col = ("y", "x"), ("z", "core")
    return jax.shard_map(
        on_device,
        mesh=torus,
        in_specs=(P(row, col), P(row, col), P(row), P(), P(row), P(row, col), P(row, col), P(row, col)),
        out_specs=(P(row, col),) * 4,
        check_vma=False,
    )
```

```python
import jax
import jax.numpy as jnp
from jax import lax
from jax.experimental import pallas as pl
from jax.experimental.pallas import tpu as pltpu
from jax.sharding import Mesh
from jax.sharding import PartitionSpec as P

BLOCK = 128
WORK = 4
CAP = 6
MOVES = 16
NX, NY, NZ = 4, 8, 8
ROWS = 64
HID = 512
PART = HID // 2
COLS = 3 * PART
RANK = WORK * BLOCK
MAIN = 384
MSG = 4 * BLOCK + 16
YMSG = 2 * BLOCK + 16
CUT = {"a": (0, 384), "b": (384, 384)}
LINKS = ("x+", "x-", "y+", "y-", "z+", "z-", "core", "pair")
RING = 6
MESH = pl.DeviceIdType.MESH
BF16, F32 = jnp.bfloat16, jnp.float32


def choose(y, x, pair, counts, moves):
    me = y * NX + x
    count = counts[0]
    zero, one = jnp.int32(0), jnp.int32(1)
    src = [moves[0, m] for m in range(MOVES)]
    dst = [moves[1, m] for m in range(MOVES)]
    blk = [moves[2, m] for m in range(MOVES)]
    src_y = [lax.div(v, jnp.int32(NX)) for v in src]
    src_x = [v - NX * w for v, w in zip(src, src_y)]

    def factor(flag):
        return jnp.where(flag, 1.0, 0.0).astype(F32)

    left = zero
    leaving = [-one] * 2
    arrives = zero
    for m in range(MOVES):
        mine = src[m] == me
        for j in range(2):
            leaving[j] = jnp.where(mine & (left == j), blk[m], leaving[j])
        left = left + jnp.where(mine, one, zero)
        arrives = arrives | jnp.where(dst[m] == me, one, zero)
    kept = zero
    chosen = [-one] * WORK
    for b in range(CAP):
        stays = (b * BLOCK < count) & (leaving[0] != b) & (leaving[1] != b)
        for s in range(WORK):
            chosen[s] = jnp.where(stays & (kept == s), jnp.int32(b), chosen[s])
        kept = kept + jnp.where(stays, one, zero)
    stay = [[factor(chosen[s] == b) for b in range(CAP)] for s in range(WORK)]
    leave = [[factor(leaving[j] == b) for b in range(CAP)] for j in range(2)]

    second = [zero] * MOVES
    for m in range(MOVES):
        for before in range(m):
            second[m] = second[m] | jnp.where(src[before] == src[m], one, zero)
    route = []
    for to_x in (x, pair):
        for d in range(NY):
            at = -one
            for m in range(MOVES):
                hit = (src_y[m] == y) & (dst[m] == d * NX + to_x)
                at = jnp.where(hit, src_x[m] * 2 + second[m], at)
            route.append([factor(at == i) for i in range(2 * NX)])
    slot = [factor((arrives == 1) & (kept == s)) for s in range(WORK)]
    return stay, leave, route, slot


def blend(factors, blocks):
    total = None
    for f, block in zip(factors, blocks):
        term = block * f.astype(BF16)
        total = term if total is None else total + term
    return total


class Graph:
    def __init__(self):
        self.nodes = {}

    def send(self, name, link, size, needs, make, silent):
        self.nodes[name] = ("send", link, size, tuple(needs), make, silent)

    def work(self, name, cost, rank, needs, run):
        self.nodes[name] = ("work", cost, rank, tuple(needs), run)

    rate, lag = 46.6e3, 2.5
    early, late = 0.6, 1.0

    def span(self, n):
        node = self.nodes[n]
        if node[0] == "work":
            return node[1]
        quick = node[1] == "core"
        return node[2] / (self.rate * (12 if quick else 1)) + (1.0 if quick else self.lag)

    def order(self):
        nodes = self.nodes
        after = {n: [] for n in nodes}
        for n, node in nodes.items():
            for m in node[3]:
                after[m].append(n)
        below = {}

        def urgency(n):
            if n not in below:
                below[n] = self.span(n) + max([urgency(m) for m in after[n]], default=0.0)
            return below[n]

        todo = sorted(nodes, key=lambda n: -urgency(n))
        done, flying, free, now, steps, times = set(), [], {}, 0.0, [], {}
        while todo or flying:
            landed = ("fin", ("my", 1)) in done
            for name in [n for n in todo if nodes[n][0] == "send"]:
                _, link, size, needs = nodes[name][:4]
                ways = ("x+", "x-") if link == "pair" else (link,)
                ahead = self.late if landed or link in ("z+", "z-", "core") else self.early
                begin = max([now] + [free.get(way, 0.0) for way in ways])
                if all(n in done for n in needs) and begin - now < ahead:
                    quick = link == "core"
                    ends = begin + size / (self.rate * (12 if quick else 1))
                    for way in ways:
                        free[way] = ends
                    flying.append((ends + (1.0 if quick else self.lag), len(steps), name))
                    steps.append(("start", name))
                    todo.remove(name)
            flying.sort()
            if flying and flying[0][0] <= now:
                name = flying.pop(0)[2]
                if not nodes[name][5]:
                    steps.append(("wait", name))
                times[name] = now
                done.add(name)
                continue
            ready = [n for n in todo if nodes[n][0] == "work" and all(m in done for m in nodes[n][3])]
            if ready:
                steps.append(("run", ready[0]))
                now += nodes[ready[0]][1]
                times[ready[0]] = now
                done.add(ready[0])
                todo.remove(ready[0])
                continue
            if flying:
                now = flying[0][0]
        times["end"] = now
        self.times = times
        return steps


def big_kernel(counts, moves, seg, tok, grad, gate, up, down, hidden_out, sums_hbm,
               w, z, xt, acc, act, tb, tb2, slots_a, slots_o, slots_s, slots_y, slots_m, xbuf, ysend, own3, tokv, gradv,
               marks, hbuf, hidden, sums_out, send_sem, recv_sem, own_sem):
    y, x = lax.axis_index("y"), lax.axis_index("x")
    zz, core = lax.axis_index("z"), lax.axis_index("core")
    size_of = {"x": NX, "y": NY, "z": NZ}
    mine = {"x": x, "y": y, "z": zz}
    side = lax.rem(x, 2)
    pair = x + 1 - 2 * side

    def step(axis, by):
        return lax.rem(mine[axis] + (by % size_of[axis]), size_of[axis])

    barrier = pltpu.get_barrier_semaphore()
    peers = [{axis: step(axis, by)} for axis in ("x", "y", "z") for by in (1, -1)] + [{"core": 1 - core}]
    for peer in peers:
        pl.semaphore_signal(barrier, inc=1, device_id=peer, device_id_type=MESH)

    own_rows = pl.ds(pl.multiple_of((y * NX + x) * ROWS, ROWS), ROWS)
    feature = zz * 2 + core
    local_rows = [
        pltpu.make_async_copy(tok, tokv, own_sem.at[0]),
        pltpu.make_async_copy(grad, gradv, own_sem.at[1]),
    ]
    local = [
        pltpu.make_async_copy(
            ref.at[:, pl.ds(p * PART, PART)], w.at[p, own_rows, pl.ds(i * PART, PART)], own_sem.at[2 + 2 * i + p]
        )
        for i, ref in enumerate((gate, up, down))
        for p in range(2)
    ]
    for copy in local_rows + local:
        copy.start()
    stay, leave, route, slot_of = choose(y, x, pair, counts, moves)

    graph = Graph()
    index = {}

    def remote(name, link, size, needs, peer, views, shared=None):
        i = index.setdefault(shared or name, len(index))

        def make(receiver, at=0):
            source, target = views(receiver)
            return pltpu.make_async_remote_copy(
                src_ref=source, dst_ref=target, send_sem=send_sem.at[at], recv_sem=recv_sem.at[i],
                device_id=peer, device_id_type=MESH,
            )

        graph.send(name, link, size, needs, make, shared is not None)

    def join(shared, members, ref):
        def wait():
            pltpu.make_async_copy(ref(), ref(), recv_sem.at[index[shared]]).wait()

        graph.work(shared, 0.0, 0, members, wait)

    def spread(tag, axis, size, needs, piece):
        n = size_of[axis]
        arrived = {0: list(needs)}
        far = (tag, "far")
        for hop in range(1, n // 2 + 1):
            for sign in (1, -1):
                part = None if hop < n // 2 else (0 if sign > 0 else 1)

                def views(receiver, sign=sign, hop=hop, part=part):
                    ref = piece(step(axis, -sign * (hop if receiver else hop - 1)), part)
                    return ref, ref

                remote((tag, sign, hop), axis + "-+"[sign > 0], size if part is None else size // 2,
                       needs if hop == 1 else [(tag, sign, hop - 1)], {axis: step(axis, sign)}, views,
                       None if part is None else far)
                if part is None:
                    arrived[sign * hop % n] = [(tag, sign, hop)]
        join(far, [(tag, 1, n // 2), (tag, -1, n // 2)], lambda: piece(step(axis, n // 2), None))
        arrived[n // 2] = [far]
        return arrived

    def x_spread(tag, size, needs, other_needs, piece):
        far = (tag, "far")
        for sign in (1, -1):
            part = 0 if sign > 0 else 1
            for hop in (1, 2):
                def same(receiver, sign=sign, hop=hop, part=part):
                    origin = step("x", -sign * (hop if receiver else hop - 1))
                    ref = piece(origin, lax.rem(origin, 2), part)
                    return ref, ref

                remote((tag, sign, hop), "x" + "-+"[sign > 0], size // 2, needs if hop == 1 else [(tag, sign, 1)],
                       {"x": step("x", sign)}, same, None if hop == 1 else far)

            def other(receiver, sign=sign):
                origin = step("x", -sign if receiver else 0)
                ref = piece(origin, 1 - lax.rem(origin, 2), None)
                return ref, ref

            remote((tag, sign, 0), "x" + "-+"[sign > 0], size, other_needs, {"x": step("x", sign)}, other)
        join(far, [(tag, 1, 2), (tag, -1, 2)], lambda: piece(step("x", 2), side, None))
        return {0: list(needs), 1: [(tag, 1, 0)], 3: [(tag, -1, 0)], 2: [far]}

    def gather_sum(tag, axis, size, own_ready, piece, cost, finish, pool, halves):
        n = size_of[axis]
        slot = {}
        slots, used = pool
        for hop in range(n // 2, 0, -1):
            for sign in (1, -1):
                name = (tag, sign, hop)
                part = None if hop < n // 2 else (0 if sign > 0 else 1)
                slot[sign, hop] = ref = slots.at[len(used)]
                used.append(name)
                if part is not None:
                    ref = halves(ref, part)

                def views(receiver, sign=sign, hop=hop, part=part, ref=ref):
                    return piece(step(axis, sign * hop), part), ref

                needs = own_ready(sign * hop % n) if hop == n // 2 else [("add", tag, sign, hop)]
                remote(name, axis + "-+"[sign > 0], size if part is None else size // 2, needs,
                       {axis: step(axis, sign)}, views)
                if hop > 1:

                    def add(sign=sign, hop=hop, part=part, ref=ref):
                        into = piece(step(axis, sign * (hop - 1)), part)
                        into[...] = (into[...].astype(F32) + ref[...].astype(F32)).astype(BF16)

                    graph.work(("add", tag, sign, hop - 1), cost, 0,
                               [name] + own_ready(sign * (hop - 1) % n), add)

        def fin():
            finish(piece(mine[axis], None), slot[1, 1], slot[-1, 1])

        graph.work(("fin", tag), 1.5 * cost, 0, [(tag, 1, 1), (tag, -1, 1)] + own_ready(0), fin)

    def x_sum(tag, size, own_ready, piece, finish, at):
        for sign in (1, -1):
            part = 0 if sign > 0 else 1
            way, peer = "x" + "-+"[sign > 0], {"x": step("x", sign)}
            first, second = slots_s.at[at, 2 * part], slots_s.at[at, 2 * part + 1]
            remote((tag, sign, 2), way, size // 2, own_ready(2), peer,
                   lambda r, part=part, first=first: (piece(step("x", 2), part), first))
            remote((tag, sign, 1), way, size // 2, [(tag, sign, 2)], peer,
                   lambda r, first=first, second=second: (first, second))
            remote((tag, sign, 0), way, size, own_ready(sign % NX), peer,
                   lambda r, sign=sign, part=part: (piece(step("x", sign), None), slots_o.at[at, part]))

        def fin():
            own_ref = piece(x, None)
            own = own_ref[...].astype(F32)
            two_on = jnp.concatenate([slots_s[at, 1], slots_s[at, 3]], axis=0).astype(F32)
            finish(own + two_on, slots_o[at, 0].astype(F32) + slots_o[at, 1].astype(F32))

        graph.work(("fin", tag), 0.15, 0, [(tag, s, h) for s in (1, -1) for h in (1, 0)] + own_ready(0), fin)

    pool_a, pool_y, pool_m = (slots_a, []), (slots_y, []), (slots_m, [])

    def prepare():
        lane = lax.broadcasted_iota(jnp.int32, (8, BLOCK), 1)
        line = lax.broadcasted_iota(jnp.int32, (8, BLOCK), 0)
        now = jnp.concatenate([seg[...], seg[0:2, :]], axis=0)
        down_one = jnp.concatenate([now[1:8, :], now[0:1, :]], axis=0)
        after = jnp.where(lane == BLOCK - 1, down_one[:, 0:1], pltpu.roll(now, BLOCK - 1, 1))
        keep = jnp.where((line * BLOCK + lane + 1 < counts[0]) & (after == now), 1.0, 0.0).astype(F32)
        marks[...] = jnp.zeros_like(marks)
        marks[pl.ds(0, 8), :] = keep
        columns = marks[...].T
        for copy in local_rows:
            copy.wait()
        for b in range(CAP):
            at = pl.ds(b * BLOCK, BLOCK)
            gradv[at, :] = (gradv[at, :].astype(F32) * columns[:, b : b + 1]).astype(BF16)
        blocks = [pl.ds(b * BLOCK, BLOCK) for b in range(CAP)]
        first_row = pl.multiple_of(x * MSG, 16)
        for t, ref in enumerate((tokv, gradv)):
            for j in range(2):
                xbuf[pl.ds(first_row + (2 * j + t) * BLOCK, BLOCK), :] = blend(leave[j], [ref[at, :] for at in blocks])
        total = jnp.sum(jnp.sum(keep, axis=0, keepdims=True), axis=1, keepdims=True)
        high = jnp.floor(total * (1 / 256))
        middle = jnp.floor((total - 256.0 * high) * (1 / 16))
        low = total - 256.0 * high - 16.0 * middle
        row = lax.broadcasted_iota(jnp.int32, (16, BLOCK), 0) - 3 * x
        digits = jnp.where(row == 0, high, jnp.where(row == 1, middle, jnp.where(row == 2, low, 0.0)))
        xbuf[pl.ds(first_row + 4 * BLOCK, 16), :] = digits.astype(BF16)

    def rank_rows(of, lo, n):
        return pl.ds(pl.multiple_of(of * RANK + lo, BLOCK), n)

    def prepare_own():
        blocks = [pl.ds(b * BLOCK, BLOCK) for b in range(CAP)]
        for t, ref in enumerate((tokv, gradv)):
            for s in range(WORK):
                rows = blend(stay[s][s:], [ref[at, :] for at in blocks[s:]])
                if s < WORK - 1:
                    z[feature, t, rank_rows(side, s * BLOCK, BLOCK), :] = rows
                else:
                    own3[0, t] = rows

    graph.work("own", 0.3, 0, [], prepare_own)

    def message(o, part):
        lo, n = (0, MSG) if part is None else ((0, 2 * BLOCK), (2 * BLOCK, MSG - 2 * BLOCK))[part]
        return xbuf.at[pl.ds(pl.multiple_of(o * MSG + lo, 16), n), :]

    mx = spread("mx", "x", MSG * BLOCK * 2, [], message)

    def select(which):
        if which == 0:
            digits = sum(xbuf[pl.ds(i * MSG + 4 * BLOCK, 16), :].astype(F32) for i in range(NX)).astype(BF16)
        else:
            digits = jnp.zeros((16, BLOCK), BF16)
        for d in range(NY):
            for t in range(2):
                blocks = [xbuf[pl.ds(i // 2 * MSG + (i % 2 * 2 + t) * BLOCK, BLOCK), :] for i in range(2 * NX)]
                ysend[which, d, pl.ds(t * BLOCK, BLOCK), :] = blend(route[which * NY + d], blocks)
            ysend[which, d, pl.ds(2 * BLOCK, 16), :] = digits

    move_halves = (pl.ds(0, BLOCK), pl.ds(BLOCK, BLOCK + 16))
    cut_move = lambda ref, part: ref.at[move_halves[part], :]
    remote("own3", "pair", 2 * BLOCK * BLOCK * 2, ["own"] + mx[1] + mx[3], {"x": pair}, lambda r: (own3.at[0], own3.at[1]))
    for which in range(2):
        graph.work(("select", which), 0.6, 0, [n for names in mx.values() for n in names], lambda which=which: select(which))

        def merge(own_ref, one, other, which=which):
            total = own_ref[...].astype(F32) + one[...].astype(F32) + other[...].astype(F32)
            of = side if which == 0 else 1 - side
            for t in range(2):
                z[feature, t, rank_rows(of, MAIN, BLOCK), :] = (
                    total[t * BLOCK : (t + 1) * BLOCK] + own3[which, t].astype(F32)
                ).astype(BF16)
            own_ref[...] = total.astype(BF16)

        ready = [("select", which), "own"] + (["own3"] if which else [])
        gather_sum(("my", which), "y", YMSG * BLOCK * 2,
                   lambda j, which=which, ready=ready: ready if j == 0 else [("select", which)],
                   lambda o, part, which=which: ysend.at[which, o] if part is None else ysend.at[which, o, move_halves[part], :],
                   0.15, merge, pool_m, cut_move)

    def loss_total():
        digits = ysend[0, y, pl.ds(2 * BLOCK, 16), :].astype(F32)
        row = lax.broadcasted_iota(jnp.int32, (16, BLOCK), 0) % 3
        parts = jnp.where(row == 0, 256.0 * digits, jnp.where(row == 1, 16.0 * digits, digits))
        return jnp.sum(parts, axis=0, keepdims=True)[:, 0:1]

    def shard_rows(at_y, at_x, part):
        first = pl.multiple_of((at_y * NX + at_x) * ROWS + (32 if part else 0), 32)
        return pl.ds(first, ROWS if part is None else 32)

    def shard(of, at_y, at_x, cut, part):
        return w.at[of, shard_rows(at_y, at_x, part), pl.ds(*CUT[cut])]

    size_a, size_b = ROWS * CUT["a"][1] * 2, ROWS * CUT["b"][1] * 2
    by_own = spread("by", "y", size_b, [], lambda o, part: shard(side, o, x, "b", part))
    by_other = spread("bz", "y", size_b, [], lambda o, part: shard(1 - side, o, x, "b", part))
    ax = x_spread("ax", size_a, mx[1] + mx[3], mx[1] + mx[3], lambda o, of, part: shard(of, y, o, "a", part))
    ay, bx = {}, {}
    for e in ax:
        ay[e] = spread(("ay", e), "y", size_a, ax[e], lambda o, part, e=e: shard(side, o, step("x", -e), "a", part))
    for f in by_own:
        bx[f] = x_spread(("bx", f), size_b, by_own[f] or mx[1] + mx[3], by_other[f] or mx[1] + mx[3],
                         lambda o, of, part, f=f: shard(of, step("y", -f), o, "b", part))

    def hand(name, lo, n, needs):
        def views(receiver):
            ref = z.at[feature, :, rank_rows(1 - side if receiver else side, lo, n), :]
            return ref, ref

        remote(name, "pair", 2 * n * BLOCK * 2, needs, {"x": pair}, views)

    hand("pm", 0, MAIN, ["own"] + mx[1] + mx[3])
    have, turns = {}, []

    def turn(c, t, of, lo, n_rows):
        rows = rank_rows(of, lo, n_rows)
        xt[t, pl.ds(pl.multiple_of(c * BLOCK, BLOCK), BLOCK), rows] = z[c, t, rows, :].T

    for tag, of, lo, rows, needs in (
        ("zm", side, 0, MAIN, ["own"]), ("zp", 1 - side, 0, MAIN, ["pm"]),
        ("zl", side, MAIN, BLOCK, [("fin", ("my", 0))]), ("zq", 1 - side, MAIN, BLOCK, [("fin", ("my", 1))]),
    ):
        have[tag] = []
        for t in range(2):
            def cut(at, part, of=of, lo=lo, rows=rows, t=t):
                if part is None:
                    return z.at[at, t, rank_rows(of, lo, rows), :]
                first = pl.multiple_of(of * RANK + lo + part * (rows // 2), 64)
                return z.at[at, t, pl.ds(first, rows // 2), :]

            size = rows * BLOCK * 2
            arrived = spread((tag, t), "z", size, needs, lambda o, part, cut=cut: cut(o * 2 + core, part))
            shared = ("core", tag, t)
            for g, names in arrived.items():
                def views(receiver, g=g, cut=cut):
                    ref = cut(step("z", -g) * 2 + (1 - core if receiver else core), None)
                    return ref, ref

                remote((shared, g), "core", size, names, {"core": 1 - core}, views, shared)
            join(shared, [(shared, g) for g in arrived],
                 lambda of=of, lo=lo, rows=rows, t=t: z.at[pl.ds(0, NZ), t, rank_rows(of, lo, rows), :])
            have[tag] += [shared] + [name for names in arrived.values() for name in names]
            for g, names in arrived.items():
                for far in range(2):
                    turns.append(("turn", tag, t, g, far))
                    graph.work(turns[-1], 0.1 if lo == 0 else 0.04, 3, [shared] if far else names,
                               lambda g=g, far=far, t=t, of=of, lo=lo, rows=rows: turn(
                                   step("z", -g) * 2 + (1 - core if far else core), t, of, lo, rows))
    last_needs = have["zl"] + have["zq"]

    seen = []

    def forward(f, tag, of):
        start = tag not in seen
        seen.append(tag)
        at = step("y", -f)
        rows = pl.ds(pl.multiple_of(at * 256, 256), 256)
        slots = rank_rows(of, 0, MAIN)
        for t, lo, n in ((0, 0, 2 * PART), (1, 2 * PART, PART)):
            left = jnp.concatenate([z[at * 2, t, slots, :], z[at * 2 + 1, t, slots, :]], axis=1)
            cols = pl.ds(lo, n)
            new = jnp.dot(left, w[side, rows, cols], preferred_element_type=F32)
            acc[slots, cols] = new if start else acc[slots, cols] + new

    last_rows = [pl.ds(p * RANK + MAIN, BLOCK) for p in range(2)]

    def forward_last():
        for t, lo, hi in ((0, 0, 2), (1, 2, 3)):
            left = jnp.concatenate(
                [jnp.concatenate([z[c, t, slots, :] for c in range(2 * NZ)], axis=1) for slots in last_rows], axis=0
            )

            def tile(n, _, left=left):
                cols = pl.ds(pl.multiple_of(n * PART, PART), PART)
                new = jnp.dot(left, w[side, :, cols], preferred_element_type=F32)
                for p, slots in enumerate(last_rows):
                    acc[slots, cols] = new[p * BLOCK : (p + 1) * BLOCK]
                return 0

            lax.fori_loop(lo, hi, tile, 0)

    all_landed = []
    for f in range(NY):
        landed = [n for e in ay for n in ay[e][f]] + [n for e in bx[f] for n in bx[f][e]]
        all_landed += landed
        for tag, of in (("zm", side), ("zp", 1 - side)):
            graph.work(("fwd", tag, f), 0.6, 2, have[tag] + landed, lambda f=f, tag=tag, of=of: forward(f, tag, of))
    graph.work("fwd last", 1.3, 2, last_needs + all_landed, forward_last)

    def pointwise():
        def rows_of(i, _):
            rows = pl.ds(pl.multiple_of(i * 64, 64), 64)
            g, u, b = acc[rows, 0:PART], acc[rows, PART : 2 * PART], acc[rows, 2 * PART : COLS]
            logistic = jax.nn.sigmoid(g)
            activated = g * logistic
            act[rows, 0:PART] = (b * u * logistic * (1.0 + g * (1.0 - logistic))).astype(BF16)
            act[rows, PART : 2 * PART] = (b * activated).astype(BF16)
            act[rows, 2 * PART : COLS] = (activated * u).astype(BF16)
            return 0

        lax.fori_loop(0, 16, rows_of, 0)

    graph.work("pointwise", 0.6, 2, [("fwd", tag, f) for tag in ("zm", "zp") for f in range(NY)] + ["fwd last"] + turns, pointwise)

    for i in range(WORK):
        def views(receiver, i=i):
            here = act.at[rank_rows(1 - side, i * BLOCK, BLOCK), pl.ds(2 * PART, PART)]
            return here, hbuf.at[pl.ds(i * BLOCK, BLOCK), :]

        remote(("hidden", i), "pair", BLOCK * PART * 2, [("bwd", 0)] if i else ["pointwise"], {"x": pair}, views)

    def store_hidden():
        stays = 1.0 - (slot_of[0] + slot_of[1] + slot_of[2])
        for which in range(2):
            cols = pl.ds(pl.multiple_of((side if which == 0 else 1 - side) * PART, PART), PART)

            def rows(s, which=which):
                if which == 0:
                    return act[rank_rows(side, s * BLOCK, BLOCK), 2 * PART : COLS]
                return hbuf[pl.ds(s * BLOCK, BLOCK), :]

            last = rows(WORK - 1)
            for s in range(WORK - 1):
                hidden[pl.ds(s * BLOCK, BLOCK), cols] = rows(s) + last * slot_of[s].astype(BF16)
            hidden[pl.ds(MAIN, BLOCK), cols] = last * stays.astype(BF16)

    hidden_copy = pltpu.make_async_copy(hidden, hidden_out, own_sem.at[8])
    sums_copy = pltpu.make_async_copy(sums_out, sums_hbm, own_sem.at[9])
    graph.work("store hidden", 0.3, 9, [("hidden", i) for i in range(WORK)], store_hidden)
    graph.work("send hidden", 0.0, 9, ["store hidden"], hidden_copy.start)

    def backward(j):
        rows = pl.ds(pl.multiple_of(step("y", j) * 256, 256), 256)
        for t, lo, n in ((0, 0, 2 * PART), (1, 2 * PART, PART)):
            cols = pl.ds(lo, n)
            tb[rows, cols] = jnp.dot(xt[t, rows, :], act[:, cols], preferred_element_type=F32).astype(BF16)

    for i, j in enumerate((4, 5, 3, 6, 2, 7, 1, 0)):
        graph.work(("bwd", j), 0.9, 1 + i, ["pointwise"], lambda j=j: backward(j))

    def plain(own_ref, one, other):
        own_ref[...] = (own_ref[...].astype(F32) + one[...].astype(F32) + other[...].astype(F32)).astype(BF16)

    def final_a(same, other):
        total = loss_total()
        sums_out[side, :, pl.ds(*CUT["a"])] = same / total
        sums_out[1 - side, :, pl.ds(*CUT["a"])] = other / total

    def final_b(p):
        def run(own_ref, one, other):
            sums = own_ref[...].astype(F32) + one[...].astype(F32) + other[...].astype(F32)
            sums_out[p, :, pl.ds(*CUT["b"])] = sums / loss_total()
        return run

    def term(at_y, at_x, cut, part):
        return tb.at[shard_rows(at_y, at_x, part), pl.ds(*CUT[cut])]

    row_halves = (pl.ds(0, 32), pl.ds(32, 32))
    for e in (2, 1, 3, 0):
        gather_sum(("say", e), "y", size_a, lambda j: [("bwd", j)],
                   lambda o, part, e=e: term(o, step("x", e), "a", part), 0.1, plain, pool_a,
                   lambda ref, part: ref.at[row_halves[part], :])
    for f in (4, 5, 3, 6, 2, 7, 1, 0):
        def keep(same, other, f=f):
            at = step("y", f)
            tb2[at, side] = same.astype(BF16)
            tb2[at, 1 - side] = other.astype(BF16)

        x_sum(("sbx", f), size_b, lambda e, f=f: [("bwd", f)],
              lambda o, part, f=f: term(step("y", f), o, "b", part), keep, f)
    x_sum("sax", size_a, lambda e: [("fin", ("say", e))], lambda o, part: term(y, o, "a", part), final_a, NY)

    for p in range(2):
        gather_sum(("sby", p), "y", size_b, lambda j: [("fin", ("sbx", j))],
                   lambda o, part, p=p: tb2.at[o, p] if part is None else tb2.at[o, p, row_halves[part], :], 0.1,
                   final_b(p), pool_y, lambda ref, part: ref.at[row_halves[part], :])

    prepare()
    for copy in local:
        copy.wait()
    pl.semaphore_wait(barrier, len(peers))
    started = {link: [] for link in LINKS}
    for kind, name in graph.order():
        node = graph.nodes[name]
        if kind == "run":
            node[4]()
        elif kind == "start":
            mates = started[node[1]]
            if len(mates) >= RING:
                mates[-RING].wait_send()
            copy = node[4](False, LINKS.index(node[1]) * RING + len(mates) % RING)
            copy.start()
            mates.append(copy)
        else:
            node[4](True).wait_recv()
    sums_copy.start()
    for mates in started.values():
        for copy in mates[-RING:]:
            copy.wait_send()
    hidden_copy.wait()
    sums_copy.wait()
    assert len(index) == RECEIVES


RECEIVES = 278


def big(counts, moves, seg, tok, grad, gate, up, down):
    vmem, smem = pl.BlockSpec(memory_space=pltpu.VMEM), pl.BlockSpec(memory_space=pltpu.SMEM)
    anyw = pl.BlockSpec(memory_space=pl.ANY)
    width = NX * NY * ROWS
    wide_a, wide_b = CUT["a"][1], CUT["b"][1]
    return pl.pallas_call(
        big_kernel,
        out_shape=(jax.ShapeDtypeStruct((RANK, HID), BF16), jax.ShapeDtypeStruct((2, ROWS, COLS), F32)),
        in_specs=[smem, smem, vmem] + [anyw] * 5,
        out_specs=(anyw,) * 2,
        scratch_shapes=[
            pltpu.VMEM((2, width, COLS), BF16),
            pltpu.VMEM((2 * NZ, 2, 2 * RANK, BLOCK), BF16),
            pltpu.VMEM((2, width, 2 * RANK), BF16),
            pltpu.VMEM((2 * RANK, COLS), F32),
            pltpu.VMEM((2 * RANK, COLS), BF16),
            pltpu.VMEM((width, COLS), BF16),
            pltpu.VMEM((NY, 2, ROWS, wide_b), BF16),
            pltpu.VMEM((32, ROWS, wide_a), BF16),
            pltpu.VMEM((NY + 1, 2, ROWS, wide_b), BF16),
            pltpu.VMEM((NY + 1, 4, ROWS // 2, wide_b), BF16),
            pltpu.VMEM((16, ROWS, wide_b), BF16),
            pltpu.VMEM((16, YMSG, BLOCK), BF16),
            pltpu.VMEM((NX * MSG, BLOCK), BF16),
            pltpu.VMEM((2, NY, YMSG, BLOCK), BF16),
            pltpu.VMEM((2, 2, BLOCK, BLOCK), BF16),
            pltpu.VMEM((CAP * BLOCK, BLOCK), BF16),
            pltpu.VMEM((CAP * BLOCK, BLOCK), BF16),
            pltpu.VMEM((BLOCK, BLOCK), F32),
            pltpu.VMEM((RANK, PART), BF16),
            pltpu.VMEM((RANK, HID), BF16),
            pltpu.VMEM((2, ROWS, COLS), F32),
            pltpu.SemaphoreType.DMA((RING * len(LINKS),)),
            pltpu.SemaphoreType.DMA((RECEIVES,)),
            pltpu.SemaphoreType.DMA((10,)),
        ],
        compiler_params=pltpu.CompilerParams(
            collective_id=0, has_side_effects=True, vmem_limit_bytes=60 * 1024 * 1024
        ),
    )(counts, moves, seg, tok, grad, gate, up, down)


def finish_kernel(hidden_in, sums, hidden, gate_out, up_out, down_out, rows, grads, sems):
    quarter = RANK // 4
    ins = [
        pltpu.make_async_copy(hidden_in.at[pl.ds(i * quarter, quarter), :], rows.at[pl.ds(i * quarter, quarter), :], sems.at[i])
        for i in range(4)
    ]
    ins += [
        pltpu.make_async_copy(
            sums.at[p, :, pl.ds(i * PART, PART)], grads.at[i, :, pl.ds(p * PART, PART)], sems.at[4 + 2 * i + p]
        )
        for i in range(3)
        for p in range(2)
    ]
    outs = [
        pltpu.make_async_copy(rows.at[pl.ds(i * quarter, quarter), :], hidden.at[pl.ds(i * quarter, quarter), :], sems.at[10 + i])
        for i in range(4)
    ]
    outs += [pltpu.make_async_copy(grads.at[i], ref, sems.at[14 + i]) for i, ref in enumerate((gate_out, up_out, down_out))]
    for copy in ins:
        copy.start()
    for i in range(4):
        ins[i].wait()
        outs[i].start()
    for i in range(3):
        ins[4 + 2 * i].wait()
        ins[5 + 2 * i].wait()
        outs[4 + i].start()
    for copy in outs:
        copy.wait()


def finish(hidden, sums):
    anyw = pl.BlockSpec(memory_space=pl.ANY)
    grad = jax.ShapeDtypeStruct((ROWS, HID), F32)
    return pl.pallas_call(
        finish_kernel,
        out_shape=(jax.ShapeDtypeStruct(hidden.shape, BF16), grad, grad, grad),
        in_specs=[anyw] * 2,
        out_specs=(anyw,) * 4,
        scratch_shapes=[
            pltpu.VMEM(hidden.shape, BF16),
            pltpu.VMEM((3, ROWS, HID), F32),
            pltpu.SemaphoreType.DMA((17,)),
        ],
    )(hidden, sums)


def on_device(tokens, out_grad, counts, block_moves, segment_ids, gate, up, down):
    seg = segment_ids.reshape(CAP, BLOCK)
    hidden, sums = big(counts, block_moves.T, seg, tokens, out_grad, gate, up, down)
    return finish(hidden, sums)


def solution(mesh):
    torus = Mesh(mesh.devices.reshape(NY, NX, NZ, 2), ("y", "x", "z", "core"))
    row, col = ("y", "x"), ("z", "core")
    return jax.shard_map(
        on_device,
        mesh=torus,
        in_specs=(P(row, col), P(row, col), P(row), P(), P(row), P(row, col), P(row, col), P(row, col)),
        out_specs=(P(row, col),) * 4,
        check_vma=False,
    )
```

```python
import random

import jax
import jax.numpy as jnp
from jax import lax
from jax.experimental import pallas as pl
from jax.experimental.pallas import tpu as pltpu
from jax.sharding import Mesh
from jax.sharding import PartitionSpec as P

BLOCK = 128
WORK = 4
CAP = 6
MOVES = 16
NX, NY, NZ = 4, 8, 8
ROWS = 64
HID = 512
PART = HID // 2
COLS = 3 * PART
RANK = WORK * BLOCK
MAIN = 384
MSG = 2 * BLOCK + 16
YMSG = BLOCK + 16
CUT = {"a": (0, 384), "b": (384, 384)}
LINKS = ("x+", "x-", "y+", "y-", "z+", "z-", "core", "pair")
RING = 4
MESH = pl.DeviceIdType.MESH
BF16, F32 = jnp.bfloat16, jnp.float32


def factor(flag):
    return jnp.where(flag, 1.0, 0.0).astype(F32)


def choose(me, count, moves):
    zero, one = jnp.int32(0), jnp.int32(1)
    left = zero
    leaving = [-one] * 2
    arrives = zero
    for m in range(MOVES):
        mine = moves[0, m] == me
        for j in range(2):
            leaving[j] = jnp.where(mine & (left == j), moves[2, m], leaving[j])
        left = left + jnp.where(mine, one, zero)
        arrives = arrives | jnp.where(moves[1, m] == me, one, zero)
    kept = zero
    chosen = [-one] * WORK
    for b in range(CAP):
        stays = (b * BLOCK < count) & (leaving[0] != b) & (leaving[1] != b)
        for s in range(WORK):
            chosen[s] = jnp.where(stays & (kept == s), jnp.int32(b), chosen[s])
        kept = kept + jnp.where(stays, one, zero)
    stay = [[factor(chosen[s] == b) for b in range(CAP)] for s in range(WORK)]
    leave = [[factor(leaving[j] == b) for b in range(CAP)] for j in range(2)]
    slot = [factor((arrives == 1) & (kept == s)) for s in range(WORK)]
    return stay, leave, slot


def routes(y, columns, moves):
    zero, one = jnp.int32(0), jnp.int32(1)
    src = [moves[0, m] for m in range(MOVES)]
    dst = [moves[1, m] for m in range(MOVES)]
    number = []
    for m in range(MOVES):
        second = zero
        for before in range(m):
            second = second | jnp.where(src[before] == src[m], one, zero)
        here = (src[m] >= y * NX) & (src[m] < y * NX + NX)
        number.append(jnp.where(here, (src[m] - y * NX) * 2 + second, -one))
    result = []
    for to_x in columns:
        for d in range(NY):
            at = -one
            for m in range(MOVES):
                at = jnp.where(dst[m] == d * NX + to_x, number[m], at)
            result.append([factor(at == i) for i in range(2 * NX)])
    return result


def blend(factors, blocks):
    total = None
    for f, block in zip(factors, blocks):
        term = block * f.astype(BF16)
        total = term if total is None else total + term
    return total


class Graph:
    def __init__(self):
        self.nodes = {}

    def send(self, name, link, size, needs, make, silent):
        self.nodes[name] = ("send", link, size, tuple(needs), make, silent)

    def work(self, name, cost, rank, needs, run):
        self.nodes[name] = ("work", cost, rank, tuple(needs), run)

    rate, lag = 46.6e3, 2.5
    early, late, along_z = 0.6, 1.0, 1.0
    seed, noise = 0, 0.0

    def span(self, n):
        node = self.nodes[n]
        if node[0] == "work":
            return node[1]
        quick = node[1] == "core"
        return node[2] / (self.rate * (12 if quick else 1)) + (1.0 if quick else self.lag)

    def order(self):
        nodes = self.nodes
        after = {n: [] for n in nodes}
        for n, node in nodes.items():
            for m in node[3]:
                after[m].append(n)
        below = {}

        def urgency(n):
            if n not in below:
                below[n] = self.span(n) + max([urgency(m) for m in after[n]], default=0.0)
            return below[n]

        draw = random.Random(self.seed)
        moved = {n: urgency(n) + draw.uniform(0.0, self.noise) for n in nodes}
        todo = sorted(nodes, key=lambda n: -moved[n])
        done, flying, free, now, steps, times = set(), [], {}, 0.0, [], {}
        while todo or flying:
            landed = ("fin", ("my", 1, 1)) in done
            for name in [n for n in todo if nodes[n][0] == "send"]:
                _, link, size, needs = nodes[name][:4]
                ways = ("x+", "x-") if link == "pair" else (link,)
                ahead = self.along_z if link in ("z+", "z-", "core") else self.late if landed else self.early
                begin = max([now] + [free.get(way, 0.0) for way in ways])
                if all(n in done for n in needs) and begin - now < ahead:
                    quick = link == "core"
                    ends = begin + size / (self.rate * (12 if quick else 1))
                    for way in ways:
                        free[way] = ends
                    flying.append((ends + (1.0 if quick else self.lag), len(steps), name))
                    steps.append(("start", name))
                    todo.remove(name)
            flying.sort()
            if flying and flying[0][0] <= now:
                name = flying.pop(0)[2]
                if not nodes[name][5]:
                    steps.append(("wait", name))
                times[name] = now
                done.add(name)
                continue
            ready = [n for n in todo if nodes[n][0] == "work" and all(m in done for m in nodes[n][3])]
            if ready:
                steps.append(("run", ready[0]))
                now += nodes[ready[0]][1]
                times[ready[0]] = now
                done.add(ready[0])
                todo.remove(ready[0])
                continue
            if flying:
                now = flying[0][0]
        times["end"] = now
        self.times = times
        return steps


def big_kernel(counts_hbm, moves_hbm, seg_hbm, tok, grad, gate, up, down, hidden, sums_out,
               w, z, xt, acc, act, tb, tb2, slots_a, slots_o, slots_s, slots_y, slots_m, xbuf, ysend, own3, tokv, gradv,
               marks, hbuf, counts, moves, seg, send_sem, recv_sem, own_sem):
    y, x = lax.axis_index("y"), lax.axis_index("x")
    zz, core = lax.axis_index("z"), lax.axis_index("core")
    size_of = {"x": NX, "y": NY, "z": NZ}
    mine = {"x": x, "y": y, "z": zz}
    side = lax.rem(x, 2)
    pair = x + 1 - 2 * side

    def step(axis, by):
        return lax.rem(mine[axis] + (by % size_of[axis]), size_of[axis])

    barrier = pltpu.get_barrier_semaphore()
    peers = [{axis: step(axis, by)} for axis in ("x", "y", "z") for by in (1, -1)] + [{"core": 1 - core}]
    for peer in peers:
        pl.semaphore_signal(barrier, inc=1, device_id=peer, device_id_type=MESH)

    own_rows = pl.ds(pl.multiple_of((y * NX + x) * ROWS, ROWS), ROWS)
    feature = zz * 2 + core
    local_rows = [
        pltpu.make_async_copy(tok, tokv, own_sem.at[0]),
        pltpu.make_async_copy(grad, gradv, own_sem.at[1]),
    ]
    local = [
        pltpu.make_async_copy(
            ref.at[:, pl.ds(p * PART, PART)], w.at[p, own_rows, pl.ds(i * PART, PART)], own_sem.at[2 + 2 * i + p]
        )
        for i, ref in enumerate((gate, up, down))
        for p in range(2)
    ]
    small = [
        pltpu.make_async_copy(ref, held, own_sem.at[8 + i])
        for i, (ref, held) in enumerate(((counts_hbm, counts), (moves_hbm, moves), (seg_hbm, seg)))
    ]
    for copy in small + local_rows + local:
        copy.start()
    for copy in small:
        copy.wait()
    stay, leave, slot_of = choose(y * NX + x, counts[0], moves)
    route = []

    graph = Graph()
    index = {}

    def remote(name, link, size, needs, peer, views, shared=None):
        i = index.setdefault(shared or name, len(index))

        def make(receiver, at=0):
            source, target = views(receiver)
            return pltpu.make_async_remote_copy(
                src_ref=source, dst_ref=target, send_sem=send_sem.at[at], recv_sem=recv_sem.at[i],
                device_id=peer, device_id_type=MESH,
            )

        graph.send(name, link, size, needs, make, shared is not None)

    def join(shared, members, ref):
        def wait():
            pltpu.make_async_copy(ref(), ref(), recv_sem.at[index[shared]]).wait()

        graph.work(shared, 0.0, 0, members, wait)

    def spread(tag, axis, size, needs, piece, to_far=True):
        n = size_of[axis]
        arrived = {0: list(needs)}
        far = (tag, "far")
        for hop in range(1, n // 2 + to_far):
            for sign in (1, -1):
                part = None if hop < n // 2 else (0 if sign > 0 else 1)

                def views(receiver, sign=sign, hop=hop, part=part):
                    ref = piece(step(axis, -sign * (hop if receiver else hop - 1)), part)
                    return ref, ref

                remote((tag, sign, hop), axis + "-+"[sign > 0], size if part is None else size // 2,
                       needs if hop == 1 else [(tag, sign, hop - 1)], {axis: step(axis, sign)}, views,
                       None if part is None else far)
                if part is None:
                    arrived[sign * hop % n] = [(tag, sign, hop)]
        if to_far:
            join(far, [(tag, 1, n // 2), (tag, -1, n // 2)], lambda: piece(step(axis, n // 2), None))
            arrived[n // 2] = [far]
        return arrived

    def x_spread(tag, size, needs, other_needs, piece, forwarded):
        far = (tag, "far")
        for sign in (1, -1):
            part = 0 if sign > 0 else 1
            for hop in (1, 2):
                def same(receiver, sign=sign, hop=hop, part=part):
                    origin = step("x", -sign * (hop if receiver else hop - 1))
                    ref = piece(origin, lax.rem(origin, 2), part)
                    return ref, ref

                remote((tag, sign, hop), "x" + "-+"[sign > 0], size // 2, needs if hop == 1 else [(tag, sign, 1)],
                       {"x": step("x", sign)}, same, None if hop == 1 else far)

            def other(receiver, sign=sign):
                origin = step("x", -sign if receiver else 0)
                ref = piece(origin, 1 - lax.rem(origin, 2), None)
                return ref, ref

            remote((tag, sign, 0), "x" + "-+"[sign > 0], size, other_needs, {"x": step("x", sign)}, other,
                   None if forwarded else far)
        if forwarded:
            join(far, [(tag, 1, 2), (tag, -1, 2)], lambda: slots_a.at[0])
            return {0: list(needs), 1: [(tag, 1, 0)], 3: [(tag, -1, 0)], 2: [far]}
        join(far, [(tag, sign, hop) for sign in (1, -1) for hop in (0, 2)], lambda: slots_a.at[pl.ds(0, 3)])
        return {0: list(needs), 1: [far], 3: [far], 2: [far]}

    def gather_sum(tag, axis, size, own_ready, piece, cost, finish, pool, halves):
        n = size_of[axis]
        slot = {}
        slots, used = pool
        near = (tag, "near")
        for hop in range(n // 2, 0, -1):
            for sign in (1, -1):
                name = (tag, sign, hop)
                part = None if hop < n // 2 else (0 if sign > 0 else 1)
                slot[sign, hop] = ref = slots.at[len(used)]
                used.append(name)
                if part is not None:
                    ref = halves(ref, part)

                def views(receiver, sign=sign, hop=hop, part=part, ref=ref):
                    return piece(step(axis, sign * hop), part), ref

                needs = own_ready(sign * hop % n) if hop == n // 2 else [("add", tag, sign, hop)]
                remote(name, axis + "-+"[sign > 0], size if part is None else size // 2, needs,
                       {axis: step(axis, sign)}, views, None if hop > 1 else near)
                if hop > 1:

                    def add(sign=sign, hop=hop, part=part, ref=ref):
                        into = piece(step(axis, sign * (hop - 1)), part)
                        into[...] = (into[...].astype(F32) + ref[...].astype(F32)).astype(BF16)

                    graph.work(("add", tag, sign, hop - 1), cost, 0,
                               [name] + own_ready(sign * (hop - 1) % n), add)

        def fin():
            finish(piece(mine[axis], None), slot[1, 1], slot[-1, 1])

        join(near, [(tag, 1, 1), (tag, -1, 1)], lambda: slots.at[pl.ds(0, 2)])
        graph.work(("fin", tag), 1.5 * cost, 0, [near] + own_ready(0), fin)

    def x_sum(tag, size, own_ready, piece, finish, at):
        near = (tag, "near")
        for sign in (1, -1):
            part = 0 if sign > 0 else 1
            way, peer = "x" + "-+"[sign > 0], {"x": step("x", sign)}
            first, second = slots_s.at[at, 2 * part], slots_s.at[at, 2 * part + 1]
            remote((tag, sign, 2), way, size // 2, own_ready(2), peer,
                   lambda r, part=part, first=first: (piece(step("x", 2), part), first))
            remote((tag, sign, 1), way, size // 2, [(tag, sign, 2)], peer,
                   lambda r, first=first, second=second: (first, second), near)
            remote((tag, sign, 0), way, size, own_ready(sign % NX), peer,
                   lambda r, sign=sign, part=part: (piece(step("x", sign), None), slots_o.at[at, part]), near)

        def fin():
            own_ref = piece(x, None)
            own = own_ref[...].astype(F32)
            two_on = jnp.concatenate([slots_s[at, 1], slots_s[at, 3]], axis=0).astype(F32)
            finish(own + two_on, slots_o[at, 0].astype(F32) + slots_o[at, 1].astype(F32))

        join(near, [(tag, s, h) for s in (1, -1) for h in (1, 0)], lambda: slots_a.at[pl.ds(0, 3)])
        graph.work(("fin", tag), 0.15, 0, [near] + own_ready(0), fin)

    pool_a, pool_y, pool_m = (slots_a, []), (slots_y, []), (slots_m, [])

    def prepare():
        lane = lax.broadcasted_iota(jnp.int32, (8, BLOCK), 1)
        line = lax.broadcasted_iota(jnp.int32, (8, BLOCK), 0)
        now = jnp.concatenate([seg[...], seg[0:2, :]], axis=0)
        down_one = jnp.concatenate([now[1:8, :], now[0:1, :]], axis=0)
        after = jnp.where(lane == BLOCK - 1, down_one[:, 0:1], pltpu.roll(now, BLOCK - 1, 1))
        keep = jnp.where((line * BLOCK + lane + 1 < counts[0]) & (after == now), 1.0, 0.0).astype(F32)
        marks[...] = jnp.zeros_like(marks)
        marks[pl.ds(0, 8), :] = keep
        columns = marks[...].T
        for copy in local_rows:
            copy.wait()
        for b in range(CAP):
            at = pl.ds(b * BLOCK, BLOCK)
            gradv[at, :] = (gradv[at, :].astype(F32) * columns[:, b : b + 1]).astype(BF16)
        blocks = [pl.ds(b * BLOCK, BLOCK) for b in range(CAP)]
        for t, ref in enumerate((tokv, gradv)):
            for j in range(2):
                xbuf[t, x, pl.ds(j * BLOCK, BLOCK), :] = blend(leave[j], [ref[at, :] for at in blocks])
        total = jnp.sum(jnp.sum(keep, axis=0, keepdims=True), axis=1, keepdims=True)
        high = jnp.floor(total * (1 / 256))
        middle = jnp.floor((total - 256.0 * high) * (1 / 16))
        low = total - 256.0 * high - 16.0 * middle
        row = lax.broadcasted_iota(jnp.int32, (16, BLOCK), 0) - 3 * x
        digits = jnp.where(row == 0, high, jnp.where(row == 1, middle, jnp.where(row == 2, low, 0.0)))
        for t in range(2):
            xbuf[t, x, pl.ds(2 * BLOCK, 16), :] = digits.astype(BF16)

    def rank_rows(of, lo, n):
        return pl.ds(pl.multiple_of(of * RANK + lo, BLOCK), n)

    def prepare_own():
        blocks = [pl.ds(b * BLOCK, BLOCK) for b in range(CAP)]
        for t, ref in enumerate((tokv, gradv)):
            for s in range(WORK):
                rows = blend(stay[s][s:], [ref[at, :] for at in blocks[s:]])
                if s < WORK - 1:
                    z[feature, t, rank_rows(side, s * BLOCK, BLOCK), :] = rows
                else:
                    own3[0, t] = rows

    graph.work("own", 0.3, 0, [], prepare_own)

    graph.work("route", 0.5, 0, [], lambda: route.extend(routes(y, (x, pair), moves)))
    mx = []
    for t in range(2):
        def message(o, part, t=t):
            lo, n = (0, MSG) if part is None else ((0, BLOCK), (BLOCK, MSG - BLOCK))[part]
            return xbuf.at[t, o, pl.ds(lo, n), :]

        mx.append(spread(("mx", t), "x", MSG * BLOCK * 2, [], message))
    mx_first = mx[0][1] + mx[0][3] + mx[1][1] + mx[1][3]

    def select(which, t):
        digits = sum(xbuf[t, i, pl.ds(2 * BLOCK, 16), :].astype(F32) for i in range(NX)).astype(BF16)
        blocks = [xbuf[t, i // 2, pl.ds(i % 2 * BLOCK, BLOCK), :] for i in range(2 * NX)]
        for d in range(NY):
            ysend[which, t, d, pl.ds(0, BLOCK), :] = blend(route[which * NY + d], blocks)
            ysend[which, t, d, pl.ds(BLOCK, 16), :] = digits

    move_halves = (pl.ds(0, BLOCK // 2), pl.ds(BLOCK // 2, YMSG - BLOCK // 2))
    cut_move = lambda ref, part: ref.at[move_halves[part], :]
    remote("own3", "pair", 2 * BLOCK * BLOCK * 2, ["own"] + mx_first, {"x": pair}, lambda r: (own3.at[0], own3.at[1]))
    for which in range(2):
        for t in range(2):
            tag = (which, t)
            graph.work(("select", which, t), 0.3, 0, ["route"] + [n for names in mx[t].values() for n in names],
                       lambda which=which, t=t: select(which, t))

            def merge(own_ref, one, other, which=which, t=t):
                total = own_ref[...].astype(F32) + one[...].astype(F32) + other[...].astype(F32)
                of = side if which == 0 else 1 - side
                z[feature, t, rank_rows(of, MAIN, BLOCK), :] = (total[0:BLOCK] + own3[which, t].astype(F32)).astype(BF16)
                own_ref[...] = total.astype(BF16)

            ready = [("select", which, t)]
            gather_sum(("my", which, t), "y", YMSG * BLOCK * 2,
                       lambda j, which=which, ready=ready: ready + ([] if j else ["own"] + ["own3"] * which),
                       lambda o, part, which=which, t=t: ysend.at[which, t, o] if part is None
                       else ysend.at[which, t, o, move_halves[part], :],
                       0.1, merge, pool_m, cut_move)

    def loss_total():
        digits = ysend[0, 0, y, pl.ds(BLOCK, 16), :].astype(F32)
        row = lax.broadcasted_iota(jnp.int32, (16, BLOCK), 0) % 3
        parts = jnp.where(row == 0, 256.0 * digits, jnp.where(row == 1, 16.0 * digits, digits))
        return jnp.sum(parts, axis=0, keepdims=True)[:, 0:1]

    def shard_rows(at_y, at_x, part):
        first = pl.multiple_of((at_y * NX + at_x) * ROWS + (32 if part else 0), 32)
        return pl.ds(first, ROWS if part is None else 32)

    def shard(of, at_y, at_x, cut, part):
        return w.at[of, shard_rows(at_y, at_x, part), pl.ds(*CUT[cut])]

    size_a, size_b = ROWS * CUT["a"][1] * 2, ROWS * CUT["b"][1] * 2
    by_own = spread("by", "y", size_b, [], lambda o, part: shard(side, o, x, "b", part))
    by_other = spread("bz", "y", size_b, [], lambda o, part: shard(1 - side, o, x, "b", part))
    ax = x_spread("ax", size_a, mx_first, mx_first, lambda o, of, part: shard(of, y, o, "a", part), True)
    ay, bx = {}, {}
    for e in ax:
        ay[e] = spread(("ay", e), "y", size_a, ax[e], lambda o, part, e=e: shard(side, o, step("x", -e), "a", part))
    for f in by_own:
        bx[f] = x_spread(("bx", f), size_b, by_own[f] or mx_first, by_other[f] or mx_first,
                         lambda o, of, part, f=f: shard(of, step("y", -f), o, "b", part), False)

    def hand(name, lo, n, needs):
        def views(receiver):
            ref = z.at[feature, :, rank_rows(1 - side if receiver else side, lo, n), :]
            return ref, ref

        remote(name, "pair", 2 * n * BLOCK * 2, needs, {"x": pair}, views)

    hand("pm", 0, MAIN, ["own"] + mx_first)
    have, turns = {}, []

    def turn(c, t, of, lo, n_rows):
        rows = rank_rows(of, lo, n_rows)
        xt[t, pl.ds(pl.multiple_of(c * BLOCK, BLOCK), BLOCK), rows] = z[c, t, rows, :].T

    for tag, of, lo, rows, needs in (
        ("zm", side, 0, MAIN, ["own"]), ("zp", 1 - side, 0, MAIN, ["pm"]),
        ("zl", side, MAIN, BLOCK, 0), ("zq", 1 - side, MAIN, BLOCK, 1),
    ):
        have[tag] = []
        for t in range(2):
            def cut(at, part, of=of, lo=lo, rows=rows, t=t):
                if part is None:
                    return z.at[at, t, rank_rows(of, lo, rows), :]
                first = pl.multiple_of(of * RANK + lo + part * (rows // 2), 64)
                return z.at[at, t, pl.ds(first, rows // 2), :]

            size = rows * BLOCK * 2
            begin = needs if lo == 0 else [("fin", ("my", needs, t))]
            arrived = spread((tag, t), "z", size, begin, lambda o, part, cut=cut: cut(o * 2 + core, part), tag != "zp")
            if tag == "zp":

                def views(receiver, t=t):
                    ref = z.at[step("z", NZ // 2) * 2 + core, t, rank_rows(1 - side if receiver else side, 0, MAIN), :]
                    return ref, ref

                remote((tag, t, "far"), "pair", size, [(("zm", t), "far")], {"x": pair}, views)
                arrived[NZ // 2] = [(tag, t, "far")]
            shared = ("core", tag, t)
            for g, names in arrived.items():
                def views(receiver, g=g, cut=cut):
                    ref = cut(step("z", -g) * 2 + (1 - core if receiver else core), None)
                    return ref, ref

                remote((shared, g), "core", size, names, {"core": 1 - core}, views, shared)
            join(shared, [(shared, g) for g in arrived],
                 lambda of=of, lo=lo, rows=rows, t=t: z.at[pl.ds(0, NZ), t, rank_rows(of, lo, rows), :])
            have[tag] += [shared] + [name for names in arrived.values() for name in names]
            for g, names in arrived.items():
                for far in range(2):
                    turns.append(("turn", tag, t, g, far))
                    graph.work(turns[-1], 0.1 if lo == 0 else 0.04, 3, [shared] if far else names,
                               lambda g=g, far=far, t=t, of=of, lo=lo, rows=rows: turn(
                                   step("z", -g) * 2 + (1 - core if far else core), t, of, lo, rows))
    last_needs = have["zl"] + have["zq"]

    seen = []

    def forward(f, tag, of):
        start = tag not in seen
        seen.append(tag)
        at = step("y", -f)
        rows = pl.ds(pl.multiple_of(at * 256, 256), 256)
        slots = rank_rows(of, 0, MAIN)
        for t, lo, n in ((0, 0, 2 * PART), (1, 2 * PART, PART)):
            left = jnp.concatenate([z[at * 2, t, slots, :], z[at * 2 + 1, t, slots, :]], axis=1)
            cols = pl.ds(lo, n)
            new = jnp.dot(left, w[side, rows, cols], preferred_element_type=F32)
            acc[slots, cols] = new if start else acc[slots, cols] + new

    last_rows = [pl.ds(p * RANK + MAIN, BLOCK) for p in range(2)]

    def forward_last():
        for t, lo, hi in ((0, 0, 2), (1, 2, 3)):
            left = jnp.concatenate(
                [jnp.concatenate([z[c, t, slots, :] for c in range(2 * NZ)], axis=1) for slots in last_rows], axis=0
            )

            def tile(n, _, left=left):
                cols = pl.ds(pl.multiple_of(n * PART, PART), PART)
                new = jnp.dot(left, w[side, :, cols], preferred_element_type=F32)
                for p, slots in enumerate(last_rows):
                    acc[slots, cols] = new[p * BLOCK : (p + 1) * BLOCK]
                return 0

            lax.fori_loop(lo, hi, tile, 0)

    all_landed = []
    for f in range(NY):
        landed = [n for e in ay for n in ay[e][f]] + [n for e in bx[f] for n in bx[f][e]]
        all_landed += landed
        for tag, of in (("zm", side), ("zp", 1 - side)):
            graph.work(("fwd", tag, f), 0.6, 2, have[tag] + landed, lambda f=f, tag=tag, of=of: forward(f, tag, of))
    graph.work("fwd last", 1.3, 2, last_needs + all_landed, forward_last)

    def pointwise():
        def rows_of(i, _):
            rows = pl.ds(pl.multiple_of(i * 64, 64), 64)
            g, u, b = acc[rows, 0:PART], acc[rows, PART : 2 * PART], acc[rows, 2 * PART : COLS]
            logistic = jax.nn.sigmoid(g)
            activated = g * logistic
            act[rows, 0:PART] = (b * u * logistic * (1.0 + g * (1.0 - logistic))).astype(BF16)
            act[rows, PART : 2 * PART] = (b * activated).astype(BF16)
            act[rows, 2 * PART : COLS] = (activated * u).astype(BF16)
            return 0

        lax.fori_loop(0, 16, rows_of, 0)

    graph.work("pointwise", 0.6, 2, [("fwd", tag, f) for tag in ("zm", "zp") for f in range(NY)] + ["fwd last"] + turns, pointwise)

    for i in range(WORK):
        def views(receiver, i=i):
            here = act.at[rank_rows(1 - side, i * BLOCK, BLOCK), pl.ds(2 * PART, PART)]
            return here, hbuf.at[pl.ds(i * BLOCK, BLOCK), :]

        remote(("hidden", i), "pair", BLOCK * PART * 2, [("bwd", 0)] if i else ["pointwise"], {"x": pair}, views)

    def store_hidden():
        stays = 1.0 - (slot_of[0] + slot_of[1] + slot_of[2])
        for which in range(2):
            cols = pl.ds(pl.multiple_of((side if which == 0 else 1 - side) * PART, PART), PART)

            def rows(s, which=which):
                if which == 0:
                    return act[rank_rows(side, s * BLOCK, BLOCK), 2 * PART : COLS]
                return hbuf[pl.ds(s * BLOCK, BLOCK), :]

            last = rows(WORK - 1)
            for s in range(WORK - 1):
                hidden[pl.ds(s * BLOCK, BLOCK), cols] = rows(s) + last * slot_of[s].astype(BF16)
            hidden[pl.ds(MAIN, BLOCK), cols] = last * stays.astype(BF16)

    graph.work("store hidden", 0.3, 9, [("hidden", i) for i in range(WORK)], store_hidden)

    def backward(j):
        rows = pl.ds(pl.multiple_of(step("y", j) * 256, 256), 256)
        for t, lo, n in ((0, 0, 2 * PART), (1, 2 * PART, PART)):
            cols = pl.ds(lo, n)
            tb[rows, cols] = jnp.dot(xt[t, rows, :], act[:, cols], preferred_element_type=F32).astype(BF16)

    for i, j in enumerate((4, 5, 3, 6, 2, 7, 1, 0)):
        graph.work(("bwd", j), 0.9, 1 + i, ["pointwise"], lambda j=j: backward(j))

    def plain(own_ref, one, other):
        own_ref[...] = (own_ref[...].astype(F32) + one[...].astype(F32) + other[...].astype(F32)).astype(BF16)

    def final_a(same, other):
        total = loss_total()
        sums_out[side, :, pl.ds(*CUT["a"])] = same / total
        sums_out[1 - side, :, pl.ds(*CUT["a"])] = other / total

    def final_b(p):
        def run(own_ref, one, other):
            sums = own_ref[...].astype(F32) + one[...].astype(F32) + other[...].astype(F32)
            sums_out[p, :, pl.ds(*CUT["b"])] = sums / loss_total()
        return run

    def term(at_y, at_x, cut, part):
        return tb.at[shard_rows(at_y, at_x, part), pl.ds(*CUT[cut])]

    row_halves = (pl.ds(0, 32), pl.ds(32, 32))
    for e in (2, 1, 3, 0):
        gather_sum(("say", e), "y", size_a, lambda j: [("bwd", j)],
                   lambda o, part, e=e: term(o, step("x", e), "a", part), 0.1, plain, pool_a,
                   lambda ref, part: ref.at[row_halves[part], :])
    for f in (4, 5, 3, 6, 2, 7, 1, 0):
        def keep(same, other, f=f):
            at = step("y", f)
            tb2[at, side] = same.astype(BF16)
            tb2[at, 1 - side] = other.astype(BF16)

        x_sum(("sbx", f), size_b, lambda e, f=f: [("bwd", f)],
              lambda o, part, f=f: term(step("y", f), o, "b", part), keep, f)
    x_sum("sax", size_a, lambda e: [("fin", ("say", e))], lambda o, part: term(y, o, "a", part), final_a, NY)

    for p in range(2):
        gather_sum(("sby", p), "y", size_b, lambda j: [("fin", ("sbx", j))],
                   lambda o, part, p=p: tb2.at[o, p] if part is None else tb2.at[o, p, row_halves[part], :], 0.1,
                   final_b(p), pool_y, lambda ref, part: ref.at[row_halves[part], :])

    prepare()
    for copy in local:
        copy.wait()
    pl.semaphore_wait(barrier, len(peers))
    started = {link: [] for link in LINKS}
    for kind, name in graph.order():
        node = graph.nodes[name]
        if kind == "run":
            node[4]()
        elif kind == "start":
            mates = started[node[1]]
            if len(mates) >= RING:
                mates[-RING].wait_send()
            copy = node[4](False, LINKS.index(node[1]) * RING + len(mates) % RING)
            copy.start()
            mates.append(copy)
        else:
            node[4](True).wait_recv()
    for mates in started.values():
        for copy in mates[-RING:]:
            copy.wait_send()
    assert len(index) == RECEIVES, len(index)


RECEIVES = 244


def big(counts, moves, seg, tok, grad, gate, up, down):
    anyw, hbm = pl.BlockSpec(memory_space=pl.ANY), pl.BlockSpec(memory_space=pltpu.HBM)
    width = NX * NY * ROWS
    wide_a, wide_b = CUT["a"][1], CUT["b"][1]
    return pl.pallas_call(
        big_kernel,
        out_shape=(pltpu.VMEM((RANK, HID), BF16), pltpu.VMEM((2, ROWS, COLS), F32)),
        in_specs=[hbm] * 8,
        out_specs=(pl.BlockSpec(memory_space=pltpu.VMEM),) * 2,
        scratch_shapes=[
            pltpu.VMEM((2, width, COLS), BF16),
            pltpu.VMEM((2 * NZ, 2, 2 * RANK, BLOCK), BF16),
            pltpu.VMEM((2, width, 2 * RANK), BF16),
            pltpu.VMEM((2 * RANK, COLS), F32),
            pltpu.VMEM((2 * RANK, COLS), BF16),
            pltpu.VMEM((width, COLS), BF16),
            pltpu.VMEM((NY, 2, ROWS, wide_b), BF16),
            pltpu.VMEM((32, ROWS, wide_a), BF16),
            pltpu.VMEM((NY + 1, 2, ROWS, wide_b), BF16),
            pltpu.VMEM((NY + 1, 4, ROWS // 2, wide_b), BF16),
            pltpu.VMEM((16, ROWS, wide_b), BF16),
            pltpu.VMEM((32, YMSG, BLOCK), BF16),
            pltpu.VMEM((2, NX, MSG, BLOCK), BF16),
            pltpu.VMEM((2, 2, NY, YMSG, BLOCK), BF16),
            pltpu.VMEM((2, 2, BLOCK, BLOCK), BF16),
            pltpu.VMEM((CAP * BLOCK, BLOCK), BF16),
            pltpu.VMEM((CAP * BLOCK, BLOCK), BF16),
            pltpu.VMEM((BLOCK, BLOCK), F32),
            pltpu.VMEM((RANK, PART), BF16),
            pltpu.SMEM((1,), jnp.int32),
            pltpu.SMEM((3, MOVES), jnp.int32),
            pltpu.VMEM((CAP, BLOCK), jnp.int32),
            pltpu.SemaphoreType.DMA((RING * len(LINKS),)),
            pltpu.SemaphoreType.DMA((RECEIVES,)),
            pltpu.SemaphoreType.DMA((11,)),
        ],
        compiler_params=pltpu.CompilerParams(
            collective_id=0, has_side_effects=True, vmem_limit_bytes=60 * 1024 * 1024
        ),
    )(counts, moves, seg, tok, grad, gate, up, down)


def finish_kernel(hidden_in, sums, hidden, gate_out, up_out, down_out, sems):
    quarter = RANK // 4
    copies = [
        pltpu.make_async_copy(hidden_in.at[pl.ds(i * quarter, quarter), :], hidden.at[pl.ds(i * quarter, quarter), :], sems.at[i])
        for i in range(4)
    ]
    copies += [
        pltpu.make_async_copy(sums.at[p, :, pl.ds(i * PART, PART)], out.at[:, pl.ds(p * PART, PART)], sems.at[4 + 2 * i + p])
        for i, out in enumerate((gate_out, up_out, down_out))
        for p in range(2)
    ]
    for copy in copies:
        copy.start()
    for copy in copies:
        copy.wait()


def finish(hidden, sums):
    anyw = pl.BlockSpec(memory_space=pl.ANY)
    grad = jax.ShapeDtypeStruct((ROWS, HID), F32)
    return pl.pallas_call(
        finish_kernel,
        out_shape=(jax.ShapeDtypeStruct(hidden.shape, BF16), grad, grad, grad),
        in_specs=[anyw] * 2,
        out_specs=(pl.BlockSpec(memory_space=pltpu.HBM),) * 4,
        scratch_shapes=[pltpu.SemaphoreType.DMA((10,))],
        compiler_params=pltpu.CompilerParams(vmem_limit_bytes=1024 * 1024),
    )(hidden, sums)


def on_device(tokens, out_grad, counts, block_moves, segment_ids, gate, up, down):
    seg = segment_ids.reshape(CAP, BLOCK)
    hidden, sums = big(counts, block_moves.T, seg, tokens, out_grad, gate, up, down)
    return finish(hidden, sums)


def solution(mesh):
    torus = Mesh(mesh.devices.reshape(NY, NX, NZ, 2), ("y", "x", "z", "core"))
    row, col = ("y", "x"), ("z", "core")
    return jax.shard_map(
        on_device,
        mesh=torus,
        in_specs=(P(row, col), P(row, col), P(row), P(), P(row), P(row, col), P(row, col), P(row, col)),
        out_specs=(P(row, col),) * 4,
        check_vma=False,
    )
```

```python
import random

import jax
import jax.numpy as jnp
from jax import lax
from jax.experimental import pallas as pl
from jax.experimental.pallas import tpu as pltpu
from jax.sharding import Mesh
from jax.sharding import PartitionSpec as P

BLOCK = 128
WORK = 4
CAP = 6
MOVES = 16
NX, NY, NZ = 4, 8, 8
ROWS = 64
HID = 512
PART = HID // 2
COLS = 3 * PART
RANK = WORK * BLOCK
MAIN = 384
MSG = 2 * BLOCK + 16
YMSG = BLOCK + 16
CUT = {"a": (0, 384), "b": (384, 384)}
LOAD = {"a": (0, 512), "b": (512, 256)}
LINKS = ("x+", "x-", "y+", "y-", "z+", "z-", "core", "pair")
PAIRED = (2, 3)
RING = 4
MESH = pl.DeviceIdType.MESH
BF16, F32 = jnp.bfloat16, jnp.float32


def factor(flag):
    return jnp.where(flag, 1.0, 0.0).astype(F32)


def choose(me, count, moves):
    zero, one = jnp.int32(0), jnp.int32(1)
    left = zero
    leaving = [-one] * 2
    arrives = zero
    for m in range(MOVES):
        mine = moves[0, m] == me
        for j in range(2):
            leaving[j] = jnp.where(mine & (left == j), moves[2, m], leaving[j])
        left = left + jnp.where(mine, one, zero)
        arrives = arrives | jnp.where(moves[1, m] == me, one, zero)
    kept = zero
    chosen = [-one] * WORK
    for b in range(CAP):
        stays = (b * BLOCK < count) & (leaving[0] != b) & (leaving[1] != b)
        for s in range(WORK):
            chosen[s] = jnp.where(stays & (kept == s), jnp.int32(b), chosen[s])
        kept = kept + jnp.where(stays, one, zero)
    stay = [[factor(chosen[s] == b) for b in range(CAP)] for s in range(WORK)]
    leave = [[factor(leaving[j] == b) for b in range(CAP)] for j in range(2)]
    slot = [factor((arrives == 1) & (kept == s)) for s in range(WORK)]
    return stay, leave, slot


def routes(y, x, moves):
    zero, one = jnp.int32(0), jnp.int32(1)
    src = [moves[0, m] for m in range(MOVES)]
    dst = [moves[1, m] for m in range(MOVES)]
    number = []
    for m in range(MOVES):
        second = zero
        for before in range(m):
            second = second | jnp.where(src[before] == src[m], one, zero)
        here = (src[m] >= y * NX) & (src[m] < y * NX + NX)
        number.append(jnp.where(here, (src[m] - y * NX) * 2 + second, -one))
    result = []
    for d in range(NY):
        at = -one
        for m in range(MOVES):
            at = jnp.where(dst[m] == d * NX + x, number[m], at)
        result.append([factor(at == i) for i in range(2 * NX)])
    return result


def blend(factors, blocks):
    total = None
    for f, block in zip(factors, blocks):
        term = block * f.astype(BF16)
        total = term if total is None else total + term
    return total


class Graph:
    def __init__(self):
        self.nodes = {}

    def send(self, name, link, size, needs, make, silent):
        self.nodes[name] = ("send", link, size, tuple(needs), make, silent)

    def work(self, name, cost, rank, needs, run):
        self.nodes[name] = ("work", cost, rank, tuple(needs), run)

    rate, lag = 46.6e3, 2.5
    early, late, along_z = 0.8, 1.0, 1.0
    seed, noise = 0, 0.0

    def span(self, n):
        node = self.nodes[n]
        if node[0] == "work":
            return node[1]
        quick = node[1] == "core"
        return node[2] / (self.rate * (12 if quick else 1)) + (1.0 if quick else self.lag)

    def order(self):
        nodes = self.nodes
        after = {n: [] for n in nodes}
        for n, node in nodes.items():
            for m in node[3]:
                after[m].append(n)
        below = {}

        def urgency(n):
            if n not in below:
                below[n] = self.span(n) + max([urgency(m) for m in after[n]], default=0.0)
            return below[n]

        draw = random.Random(self.seed)
        moved = {n: urgency(n) + draw.uniform(0.0, self.noise) for n in nodes}
        todo = sorted(nodes, key=lambda n: -moved[n])
        done, flying, free, now, steps, times = set(), [], {}, 0.0, [], {}
        while todo or flying:
            landed = ("pl", 1) in done
            for name in [n for n in todo if nodes[n][0] == "send"]:
                _, link, size, needs = nodes[name][:4]
                ways = ("x+", "x-") if link == "pair" else (link,)
                ahead = self.along_z if link in ("z+", "z-", "core") else self.late if landed else self.early
                begin = max([now] + [free.get(way, 0.0) for way in ways])
                if all(n in done for n in needs) and begin - now < ahead:
                    quick = link == "core"
                    ends = begin + size / (self.rate * (12 if quick else 1))
                    for way in ways:
                        free[way] = ends
                    flying.append((ends + (1.0 if quick else self.lag), len(steps), name))
                    steps.append(("start", name))
                    todo.remove(name)
            flying.sort()
            if flying and flying[0][0] <= now:
                name = flying.pop(0)[2]
                if not nodes[name][5]:
                    steps.append(("wait", name))
                times[name] = now
                done.add(name)
                continue
            ready = [n for n in todo if nodes[n][0] == "work" and all(m in done for m in nodes[n][3])]
            if ready:
                steps.append(("run", ready[0]))
                now += nodes[ready[0]][1]
                times[ready[0]] = now
                done.add(ready[0])
                todo.remove(ready[0])
                continue
            if flying:
                now = flying[0][0]
        times["end"] = now
        self.times = times
        return steps


def big_kernel(counts_hbm, moves_hbm, seg_hbm, tok, grad, gate, up, down, hidden, sums_out,
               w, z, xt, acc, act, tb, tb2, slots_a, slots_o, slots_s, slots_y, slots_m, xbuf, ysend, own3, tokv, gradv,
               marks, hbuf, counts, moves, seg, send_sem, recv_sem, own_sem):
    y, x = lax.axis_index("y"), lax.axis_index("x")
    zz, core = lax.axis_index("z"), lax.axis_index("core")
    size_of = {"x": NX, "y": NY, "z": NZ}
    mine = {"x": x, "y": y, "z": zz}
    side = lax.rem(x, 2)
    pair = x + 1 - 2 * side

    def step(axis, by):
        return lax.rem(mine[axis] + (by % size_of[axis]), size_of[axis])

    barrier = pltpu.get_barrier_semaphore()
    peers = [{axis: step(axis, by)} for axis in ("x", "y", "z") for by in (1, -1)] + [{"core": 1 - core}]
    for peer in peers:
        pl.semaphore_signal(barrier, inc=1, device_id=peer, device_id_type=MESH)

    own_rows = pl.ds(pl.multiple_of((y * NX + x) * ROWS, ROWS), ROWS)
    feature = zz * 2 + core
    local_rows = [
        pltpu.make_async_copy(tok, tokv, own_sem.at[0]),
        pltpu.make_async_copy(grad, gradv, own_sem.at[1]),
    ]
    local = [
        pltpu.make_async_copy(
            ref.at[:, pl.ds(p * PART, PART)], w.at[p, own_rows, pl.ds(i * PART, PART)], own_sem.at[2 + 2 * i + p]
        )
        for i, ref in enumerate((gate, up, down))
        for p in range(2)
    ]
    small = [
        pltpu.make_async_copy(ref, held, own_sem.at[8 + i])
        for i, (ref, held) in enumerate(((counts_hbm, counts), (moves_hbm, moves), (seg_hbm, seg)))
    ]
    for copy in small + local_rows + local:
        copy.start()
    for copy in small:
        copy.wait()
    stay, leave, slot_of = choose(y * NX + x, counts[0], moves)
    route = []

    graph = Graph()
    index = {}

    def remote(name, link, size, needs, peer, views, shared=None):
        i = index.setdefault(shared or name, len(index))

        def make(receiver, at=0):
            source, target = views(receiver)
            return pltpu.make_async_remote_copy(
                src_ref=source, dst_ref=target, send_sem=send_sem.at[at], recv_sem=recv_sem.at[i],
                device_id=peer, device_id_type=MESH,
            )

        graph.send(name, link, size, needs, make, shared is not None)

    def join(shared, members, ref):
        def wait():
            pltpu.make_async_copy(ref(), ref(), recv_sem.at[index[shared]]).wait()

        graph.work(shared, 0.0, 0, members, wait)

    def spread(tag, axis, size, needs, piece, hops=None):
        n = size_of[axis]
        arrived = {0: list(needs)}
        far = (tag, "far")
        hops = n // 2 if hops is None else hops
        for hop in range(1, hops + 1):
            base = hop - 1
            for sign in (1, -1):
                part = None if hop < n // 2 else (0 if sign > 0 else 1)

                def views(receiver, sign=sign, hop=hop, base=base, part=part):
                    ref = piece(step(axis, -sign * (hop if receiver else base)), part)
                    return ref, ref

                share = size if part is None else size // 2
                remote((tag, sign, hop), axis + "-+"[sign > 0], share * (hop - base),
                       [(tag, sign, base)] if base else needs, {axis: step(axis, sign * (hop - base))}, views,
                       None if part is None else far)
                if part is None:
                    arrived[sign * hop % n] = [(tag, sign, hop)]
        if hops == n // 2:
            join(far, [(tag, 1, n // 2), (tag, -1, n // 2)], lambda: piece(step(axis, n // 2), None))
            arrived[n // 2] = [far]
        return arrived

    def x_spread(tag, size, needs, other_needs, piece, forwarded):
        far = (tag, "far")
        for sign in (1, -1):
            part = 0 if sign > 0 else 1
            for hop in (1, 2):
                def same(receiver, sign=sign, hop=hop, part=part):
                    origin = step("x", -sign * (hop if receiver else hop - 1))
                    ref = piece(origin, lax.rem(origin, 2), part)
                    return ref, ref

                remote((tag, sign, hop), "x" + "-+"[sign > 0], size // 2, needs if hop == 1 else [(tag, sign, 1)],
                       {"x": step("x", sign)}, same, None if hop == 1 else far)

            def other(receiver, sign=sign):
                origin = step("x", -sign if receiver else 0)
                ref = piece(origin, 1 - lax.rem(origin, 2), None)
                return ref, ref

            remote((tag, sign, 0), "x" + "-+"[sign > 0], size, other_needs, {"x": step("x", sign)}, other,
                   None if forwarded else far)
        if forwarded:
            join(far, [(tag, 1, 2), (tag, -1, 2)], lambda: w.at[0, pl.ds(0, ROWS), pl.ds(*LOAD["a"])])
            return {0: list(needs), 1: [(tag, 1, 0)], 3: [(tag, -1, 0)], 2: [far]}
        join(far, [(tag, sign, hop) for sign in (1, -1) for hop in (0, 2)],
             lambda: w.at[0, pl.ds(0, 3 * ROWS), pl.ds(*LOAD["b"])])
        return {0: list(needs), 1: [far], 3: [far], 2: [far]}

    def gather_sum(tag, axis, size, own_ready, piece, cost, finish, pool, halves):
        n = size_of[axis]
        slot = {}
        slots, used = pool
        near = (tag, "near")
        for hop in range(n // 2, 0, -1):
            for sign in (1, -1):
                name = (tag, sign, hop)
                part = None if hop < n // 2 else (0 if sign > 0 else 1)
                slot[sign, hop] = ref = slots.at[len(used)]
                used.append(name)
                if part is not None:
                    ref = halves(ref, part)

                def views(receiver, sign=sign, hop=hop, part=part, ref=ref):
                    return piece(step(axis, sign * hop), part), ref

                needs = own_ready(sign * hop % n) if hop == n // 2 else [("add", tag, sign, hop)]
                remote(name, axis + "-+"[sign > 0], size if part is None else size // 2, needs,
                       {axis: step(axis, sign)}, views, None if hop > 1 else near)
                if hop > 1:

                    def add(sign=sign, hop=hop, part=part, ref=ref):
                        into = piece(step(axis, sign * (hop - 1)), part)
                        into[...] = (into[...].astype(F32) + ref[...].astype(F32)).astype(BF16)

                    graph.work(("add", tag, sign, hop - 1), cost, 0,
                               [name] + own_ready(sign * (hop - 1) % n), add)

        def fin():
            finish(piece(mine[axis], None), slot[1, 1], slot[-1, 1])

        join(near, [(tag, 1, 1), (tag, -1, 1)], lambda: slots.at[pl.ds(0, 2)])
        graph.work(("fin", tag), 1.5 * cost, 0, [near] + own_ready(0), fin)

    def x_sum(tag, size, own_ready, piece, finish, at):
        near = (tag, "near")
        for sign in (1, -1):
            part = 0 if sign > 0 else 1
            way, peer = "x" + "-+"[sign > 0], {"x": step("x", sign)}
            first, second = slots_s.at[at, 2 * part], slots_s.at[at, 2 * part + 1]
            remote((tag, sign, 2), way, size // 2, own_ready(2), peer,
                   lambda r, part=part, first=first: (piece(step("x", 2), part), first))
            remote((tag, sign, 1), way, size // 2, [(tag, sign, 2)], peer,
                   lambda r, first=first, second=second: (first, second), near)
            remote((tag, sign, 0), way, size, own_ready(sign % NX), peer,
                   lambda r, sign=sign, part=part: (piece(step("x", sign), None), slots_o.at[at, part]), near)

        def fin():
            own_ref = piece(x, None)
            own = own_ref[...].astype(F32)
            two_on = jnp.concatenate([slots_s[at, 1], slots_s[at, 3]], axis=0).astype(F32)
            finish(own + two_on, slots_o[at, 0].astype(F32) + slots_o[at, 1].astype(F32))

        join(near, [(tag, s, h) for s in (1, -1) for h in (1, 0)], lambda: slots_a.at[pl.ds(0, 3)])
        graph.work(("fin", tag), 0.15, 0, [near] + own_ready(0), fin)

    pool_a, pool_y, pool_m = (slots_a, []), (slots_y, []), (slots_m, [])

    def prepare():
        lane = lax.broadcasted_iota(jnp.int32, (8, BLOCK), 1)
        line = lax.broadcasted_iota(jnp.int32, (8, BLOCK), 0)
        now = jnp.concatenate([seg[...], seg[0:2, :]], axis=0)
        down_one = jnp.concatenate([now[1:8, :], now[0:1, :]], axis=0)
        after = jnp.where(lane == BLOCK - 1, down_one[:, 0:1], pltpu.roll(now, BLOCK - 1, 1))
        keep = jnp.where((line * BLOCK + lane + 1 < counts[0]) & (after == now), 1.0, 0.0).astype(F32)
        marks[...] = jnp.zeros_like(marks)
        marks[pl.ds(0, 8), :] = keep
        columns = marks[...].T
        for copy in local_rows:
            copy.wait()
        for b in range(CAP):
            at = pl.ds(b * BLOCK, BLOCK)
            gradv[at, :] = (gradv[at, :].astype(F32) * columns[:, b : b + 1]).astype(BF16)
        blocks = [pl.ds(b * BLOCK, BLOCK) for b in range(CAP)]
        for t, ref in enumerate((tokv, gradv)):
            for j in range(2):
                xbuf[t, x, pl.ds(j * BLOCK, BLOCK), :] = blend(leave[j], [ref[at, :] for at in blocks])
        total = jnp.sum(jnp.sum(keep, axis=0, keepdims=True), axis=1, keepdims=True)
        high = jnp.floor(total * (1 / 256))
        middle = jnp.floor((total - 256.0 * high) * (1 / 16))
        low = total - 256.0 * high - 16.0 * middle
        row = lax.broadcasted_iota(jnp.int32, (16, BLOCK), 0) - 3 * x
        digits = jnp.where(row == 0, high, jnp.where(row == 1, middle, jnp.where(row == 2, low, 0.0)))
        for t in range(2):
            xbuf[t, x, pl.ds(2 * BLOCK, 16), :] = digits.astype(BF16)

    def rank_rows(of, lo, n):
        return pl.ds(pl.multiple_of(of * RANK + lo, BLOCK), n)

    def prepare_own():
        blocks = [pl.ds(b * BLOCK, BLOCK) for b in range(CAP)]
        for t, ref in enumerate((tokv, gradv)):
            for s in range(WORK):
                rows = blend(stay[s][s:], [ref[at, :] for at in blocks[s:]])
                if s < WORK - 1:
                    z[feature, t, rank_rows(side, s * BLOCK, BLOCK), :] = rows
                else:
                    own3[t] = rows

    graph.work("own", 0.3, 0, [], prepare_own)

    graph.work("route", 0.5, 0, [], lambda: route.extend(routes(y, x, moves)))
    mx = []
    for t in range(2):
        def message(o, part, t=t):
            lo, n = (0, MSG) if part is None else ((0, BLOCK), (BLOCK, MSG - BLOCK))[part]
            return xbuf.at[t, o, pl.ds(lo, n), :]

        mx.append(spread(("mx", t), "x", MSG * BLOCK * 2, [], message))
    mx_first = mx[0][1] + mx[0][3] + mx[1][1] + mx[1][3]

    def select(t):
        digits = sum(xbuf[t, i, pl.ds(2 * BLOCK, 16), :].astype(F32) for i in range(NX)).astype(BF16)
        blocks = [xbuf[t, i // 2, pl.ds(i % 2 * BLOCK, BLOCK), :] for i in range(2 * NX)]
        for d in range(NY):
            ysend[t, d, pl.ds(0, BLOCK), :] = blend(route[d], blocks)
            ysend[t, d, pl.ds(BLOCK, 16), :] = digits

    move_halves = (pl.ds(0, BLOCK // 2), pl.ds(BLOCK // 2, YMSG - BLOCK // 2))
    cut_move = lambda ref, part: ref.at[move_halves[part], :]
    for t in range(2):
        graph.work(("select", t), 0.3, 0, ["route"] + [n for names in mx[t].values() for n in names], lambda t=t: select(t))

        def merge(own_ref, one, other, t=t):
            total = own_ref[...].astype(F32) + one[...].astype(F32) + other[...].astype(F32)
            z[feature, t, rank_rows(side, MAIN, BLOCK), :] = (total[0:BLOCK] + own3[t].astype(F32)).astype(BF16)
            own_ref[...] = total.astype(BF16)

        gather_sum(("my", t), "y", YMSG * BLOCK * 2, lambda j, t=t: [("select", t)] + ([] if j else ["own"]),
                   lambda o, part, t=t: ysend.at[t, o] if part is None else ysend.at[t, o, move_halves[part], :],
                   0.1, merge, pool_m, cut_move)

        def handed(receiver, t=t):
            ref = z.at[feature, t, rank_rows(1 - side if receiver else side, MAIN, BLOCK), :]
            return ref, ref

        remote(("pl", t), "pair", BLOCK * BLOCK * 2, [("fin", ("my", t))], {"x": pair}, handed)

    def loss_total():
        digits = ysend[0, y, pl.ds(BLOCK, 16), :].astype(F32)
        row = lax.broadcasted_iota(jnp.int32, (16, BLOCK), 0) % 3
        parts = jnp.where(row == 0, 256.0 * digits, jnp.where(row == 1, 16.0 * digits, digits))
        return jnp.sum(parts, axis=0, keepdims=True)[:, 0:1]

    def shard_rows(at_y, at_x, part):
        first = pl.multiple_of((at_y * NX + at_x) * ROWS + (32 if part else 0), 32)
        return pl.ds(first, ROWS if part is None else 32)

    def shard(of, at_y, at_x, cut, part):
        return w.at[of, shard_rows(at_y, at_x, part), pl.ds(*LOAD[cut])]

    load_a, load_b = (ROWS * LOAD[cut][1] * 2 for cut in "ab")
    by_own = spread("by", "y", load_b, [], lambda o, part: shard(side, o, x, "b", part))
    by_other = spread("bz", "y", load_b, [], lambda o, part: shard(1 - side, o, x, "b", part))
    ax = x_spread("ax", load_a, mx_first, mx_first, lambda o, of, part: shard(of, y, o, "a", part), True)
    ay, bx = {}, {}
    for e in ax:
        ay[e] = spread(("ay", e), "y", load_a, ax[e], lambda o, part, e=e: shard(side, o, step("x", -e), "a", part))
    for f in by_own:
        bx[f] = x_spread(("bx", f), load_b, by_own[f] or mx_first, by_other[f] or mx_first,
                         lambda o, of, part, f=f: shard(of, step("y", -f), o, "b", part), False)

    def hand(name, lo, n, needs):
        def views(receiver):
            ref = z.at[feature, :, rank_rows(1 - side if receiver else side, lo, n), :]
            return ref, ref

        remote(name, "pair", 2 * n * BLOCK * 2, needs, {"x": pair}, views)

    hand("pm", 0, MAIN, ["own"] + mx_first)
    have, turns, landed_of = {}, [], {}

    def turn(c, t, of, lo, n_rows):
        rows = rank_rows(of, lo, n_rows)
        xt[t, pl.ds(pl.multiple_of(c * BLOCK, BLOCK), BLOCK), rows] = z[c, t, rows, :].T

    for tag, of, lo, rows, needs in (
        ("zm", side, 0, MAIN, ["own"]), ("zp", 1 - side, 0, MAIN, ["pm"]),
        ("zl", side, MAIN, BLOCK, []), ("zq", 1 - side, MAIN, BLOCK, []),
    ):
        have[tag] = []
        for t in range(2):
            def cut(at, part, of=of, lo=lo, rows=rows, t=t):
                if part is None:
                    return z.at[at, t, rank_rows(of, lo, rows), :]
                first = pl.multiple_of(of * RANK + lo + part * (rows // 2), 64)
                return z.at[at, t, pl.ds(first, rows // 2), :]

            size = rows * BLOCK * 2
            begin = {"zl": [("fin", ("my", t))], "zq": [("pl", t)]}.get(tag, needs)
            hops = PAIRED[t] if tag == "zp" else NZ // 2
            arrived = spread((tag, t), "z", size, begin, lambda o, part, cut=cut: cut(o * 2 + core, part), hops)
            landed_of[tag, t] = arrived
            for g in range(hops + 1, NZ - hops):

                def views(receiver, t=t, g=g):
                    ref = z.at[step("z", -g) * 2 + core, t, rank_rows(1 - side if receiver else side, 0, MAIN), :]
                    return ref, ref

                remote((tag, t, g), "pair", size, landed_of["zm", t][g], {"x": pair}, views)
                arrived[g] = [(tag, t, g)]
            shared = ("core", tag, t)
            for g, names in arrived.items():
                def views(receiver, g=g, cut=cut):
                    ref = cut(step("z", -g) * 2 + (1 - core if receiver else core), None)
                    return ref, ref

                remote((shared, g), "core", size, names, {"core": 1 - core}, views, shared)
            join(shared, [(shared, g) for g in arrived],
                 lambda of=of, lo=lo, rows=rows, t=t: z.at[pl.ds(0, NZ), t, rank_rows(of, lo, rows), :])
            have[tag] += [shared] + [name for names in arrived.values() for name in names]
            for g, names in arrived.items():
                for far in range(2):
                    turns.append(("turn", tag, t, g, far))
                    graph.work(turns[-1], 0.1 if lo == 0 else 0.04, 3, [shared] if far else names,
                               lambda g=g, far=far, t=t, of=of, lo=lo, rows=rows: turn(
                                   step("z", -g) * 2 + (1 - core if far else core), t, of, lo, rows))

    seen = []

    def forward(f, tag, of):
        start = tag not in seen
        seen.append(tag)
        at = step("y", -f)
        rows = pl.ds(pl.multiple_of(at * 256, 256), 256)
        slots = rank_rows(of, 0, MAIN)
        for t, lo, n in ((0, 0, 2 * PART), (1, 2 * PART, PART)):
            left = jnp.concatenate([z[at * 2, t, slots, :], z[at * 2 + 1, t, slots, :]], axis=1)
            cols = pl.ds(lo, n)
            new = jnp.dot(left, w[side, rows, cols], preferred_element_type=F32)
            acc[slots, cols] = new if start else acc[slots, cols] + new

    def forward_last(of):
        slots = rank_rows(of, MAIN, BLOCK)
        for t, lo, n in ((0, 0, 2 * PART), (1, 2 * PART, PART)):
            left = jnp.concatenate([z[c, t, slots, :] for c in range(2 * NZ)], axis=1)
            cols = pl.ds(lo, n)
            acc[slots, cols] = jnp.dot(left, w[side, :, cols], preferred_element_type=F32)

    all_landed = []
    for f in range(NY):
        landed = [n for e in ay for n in ay[e][f]] + [n for e in bx[f] for n in bx[f][e]]
        all_landed += landed
        for tag, of in (("zm", side), ("zp", 1 - side)):
            graph.work(("fwd", tag, f), 0.6, 2, have[tag] + landed, lambda f=f, tag=tag, of=of: forward(f, tag, of))
    for tag, of in (("zl", side), ("zq", 1 - side)):
        graph.work(("fwd last", tag), 0.8, 2, have[tag] + all_landed, lambda of=of: forward_last(of))

    def pointwise(of, lo, n):
        def rows_of(i, _):
            rows = pl.ds(pl.multiple_of(of * RANK + lo + i * 64, 64), 64)
            g, u, b = acc[rows, 0:PART], acc[rows, PART : 2 * PART], acc[rows, 2 * PART : COLS]
            logistic = jax.nn.sigmoid(g)
            activated = g * logistic
            act[rows, 0:PART] = (b * u * logistic * (1.0 + g * (1.0 - logistic))).astype(BF16)
            act[rows, PART : 2 * PART] = (b * activated).astype(BF16)
            act[rows, 2 * PART : COLS] = (activated * u).astype(BF16)
            return 0

        lax.fori_loop(0, n // 64, rows_of, 0)

    for tag, of in (("zm", side), ("zp", 1 - side)):
        graph.work(("pointwise", tag), 0.25, 2, [("fwd", tag, f) for f in range(NY)], lambda of=of: pointwise(of, 0, MAIN))
    for tag, of in (("zl", side), ("zq", 1 - side)):
        graph.work(("pointwise", tag), 0.1, 2, [("fwd last", tag)], lambda of=of: pointwise(of, MAIN, BLOCK))
    graph.work("pointwise", 0.0, 2, [("pointwise", tag) for tag in have] + turns, lambda: None)

    for i in range(WORK):
        def views(receiver, i=i):
            here = act.at[rank_rows(1 - side, i * BLOCK, BLOCK), pl.ds(2 * PART, PART)]
            return here, hbuf.at[pl.ds(i * BLOCK, BLOCK), :]

        remote(("hidden", i), "pair", BLOCK * PART * 2, [("bwd", 0)] if i else ["pointwise"], {"x": pair}, views)

    def store_hidden():
        stays = 1.0 - (slot_of[0] + slot_of[1] + slot_of[2])
        for which in range(2):
            cols = pl.ds(pl.multiple_of((side if which == 0 else 1 - side) * PART, PART), PART)

            def rows(s, which=which):
                if which == 0:
                    return act[rank_rows(side, s * BLOCK, BLOCK), 2 * PART : COLS]
                return hbuf[pl.ds(s * BLOCK, BLOCK), :]

            last = rows(WORK - 1)
            for s in range(WORK - 1):
                hidden[pl.ds(s * BLOCK, BLOCK), cols] = rows(s) + last * slot_of[s].astype(BF16)
            hidden[pl.ds(MAIN, BLOCK), cols] = last * stays.astype(BF16)

    graph.work("store hidden", 0.3, 9, [("hidden", i) for i in range(WORK)], store_hidden)

    def backward(j):
        rows = pl.ds(pl.multiple_of(step("y", j) * 256, 256), 256)
        for t, lo, n in ((0, 0, 2 * PART), (1, 2 * PART, PART)):
            cols = pl.ds(lo, n)
            tb[rows, cols] = jnp.dot(xt[t, rows, :], act[:, cols], preferred_element_type=F32).astype(BF16)

    for i, j in enumerate((4, 5, 3, 6, 2, 7, 1, 0)):
        graph.work(("bwd", j), 0.9, 1 + i, ["pointwise"], lambda j=j: backward(j))

    size_a, size_b = (ROWS * CUT[cut][1] * 2 for cut in "ab")

    def plain(own_ref, one, other):
        own_ref[...] = (own_ref[...].astype(F32) + one[...].astype(F32) + other[...].astype(F32)).astype(BF16)

    def final_a(same, other):
        total = loss_total()
        sums_out[side, :, pl.ds(*CUT["a"])] = same / total
        sums_out[1 - side, :, pl.ds(*CUT["a"])] = other / total

    def final_b(p):
        def run(own_ref, one, other):
            sums = own_ref[...].astype(F32) + one[...].astype(F32) + other[...].astype(F32)
            sums_out[p, :, pl.ds(*CUT["b"])] = sums / loss_total()
        return run

    def term(at_y, at_x, cut, part):
        return tb.at[shard_rows(at_y, at_x, part), pl.ds(*CUT[cut])]

    row_halves = (pl.ds(0, 32), pl.ds(32, 32))
    for e in (2, 1, 3, 0):
        gather_sum(("say", e), "y", size_a, lambda j: [("bwd", j)],
                   lambda o, part, e=e: term(o, step("x", e), "a", part), 0.1, plain, pool_a,
                   lambda ref, part: ref.at[row_halves[part], :])
    for f in (4, 5, 3, 6, 2, 7, 1, 0):
        def keep(same, other, f=f):
            at = step("y", f)
            tb2[at, side] = same.astype(BF16)
            tb2[at, 1 - side] = other.astype(BF16)

        x_sum(("sbx", f), size_b, lambda e, f=f: [("bwd", f)],
              lambda o, part, f=f: term(step("y", f), o, "b", part), keep, f)
    x_sum("sax", size_a, lambda e: [("fin", ("say", e))], lambda o, part: term(y, o, "a", part), final_a, NY)

    for p in range(2):
        gather_sum(("sby", p), "y", size_b, lambda j: [("fin", ("sbx", j))],
                   lambda o, part, p=p: tb2.at[o, p] if part is None else tb2.at[o, p, row_halves[part], :], 0.1,
                   final_b(p), pool_y, lambda ref, part: ref.at[row_halves[part], :])

    prepare()
    for copy in local:
        copy.wait()
    pl.semaphore_wait(barrier, len(peers))
    started = {link: [] for link in LINKS}
    for kind, name in graph.order():
        node = graph.nodes[name]
        if kind == "run":
            node[4]()
        elif kind == "start":
            mates = started[node[1]]
            if len(mates) >= RING:
                mates[-RING].wait_send()
            copy = node[4](False, LINKS.index(node[1]) * RING + len(mates) % RING)
            copy.start()
            mates.append(copy)
        else:
            node[4](True).wait_recv()
    for mates in started.values():
        for copy in mates[-RING:]:
            copy.wait_send()
    assert len(index) == RECEIVES


RECEIVES = 231


def big(counts, moves, seg, tok, grad, gate, up, down):
    anyw, hbm = pl.BlockSpec(memory_space=pl.ANY), pl.BlockSpec(memory_space=pltpu.HBM)
    width = NX * NY * ROWS
    wide_a, wide_b = CUT["a"][1], CUT["b"][1]
    return pl.pallas_call(
        big_kernel,
        out_shape=(pltpu.VMEM((RANK, HID), BF16), pltpu.VMEM((2, ROWS, COLS), F32)),
        in_specs=[hbm] * 8,
        out_specs=(pl.BlockSpec(memory_space=pltpu.VMEM),) * 2,
        scratch_shapes=[
            pltpu.VMEM((2, width, COLS), BF16),
            pltpu.VMEM((2 * NZ, 2, 2 * RANK, BLOCK), BF16),
            pltpu.VMEM((2, width, 2 * RANK), BF16),
            pltpu.VMEM((2 * RANK, COLS), F32),
            pltpu.VMEM((2 * RANK, COLS), BF16),
            pltpu.VMEM((width, COLS), BF16),
            pltpu.VMEM((NY, 2, ROWS, wide_b), BF16),
            pltpu.VMEM((32, ROWS, wide_a), BF16),
            pltpu.VMEM((NY + 1, 2, ROWS, wide_b), BF16),
            pltpu.VMEM((NY + 1, 4, ROWS // 2, wide_b), BF16),
            pltpu.VMEM((16, ROWS, wide_b), BF16),
            pltpu.VMEM((16, YMSG, BLOCK), BF16),
            pltpu.VMEM((2, NX, MSG, BLOCK), BF16),
            pltpu.VMEM((2, NY, YMSG, BLOCK), BF16),
            pltpu.VMEM((2, BLOCK, BLOCK), BF16),
            pltpu.VMEM((CAP * BLOCK, BLOCK), BF16),
            pltpu.VMEM((CAP * BLOCK, BLOCK), BF16),
            pltpu.VMEM((BLOCK, BLOCK), F32),
            pltpu.VMEM((RANK, PART), BF16),
            pltpu.SMEM((1,), jnp.int32),
            pltpu.SMEM((3, MOVES), jnp.int32),
            pltpu.VMEM((CAP, BLOCK), jnp.int32),
            pltpu.SemaphoreType.DMA((RING * len(LINKS),)),
            pltpu.SemaphoreType.DMA((RECEIVES,)),
            pltpu.SemaphoreType.DMA((11,)),
        ],
        compiler_params=pltpu.CompilerParams(
            collective_id=0, has_side_effects=True, vmem_limit_bytes=60 * 1024 * 1024
        ),
    )(counts, moves, seg, tok, grad, gate, up, down)


def finish_kernel(hidden_in, sums, hidden, gate_out, up_out, down_out, sems):
    quarter = RANK // 4
    copies = [
        pltpu.make_async_copy(hidden_in.at[pl.ds(i * quarter, quarter), :], hidden.at[pl.ds(i * quarter, quarter), :], sems.at[i])
        for i in range(4)
    ]
    copies += [
        pltpu.make_async_copy(sums.at[p, :, pl.ds(i * PART, PART)], out.at[:, pl.ds(p * PART, PART)], sems.at[4 + 2 * i + p])
        for i, out in enumerate((gate_out, up_out, down_out))
        for p in range(2)
    ]
    for copy in copies:
        copy.start()
    for copy in copies:
        copy.wait()


def finish(hidden, sums):
    anyw = pl.BlockSpec(memory_space=pl.ANY)
    grad = jax.ShapeDtypeStruct((ROWS, HID), F32)
    return pl.pallas_call(
        finish_kernel,
        out_shape=(jax.ShapeDtypeStruct(hidden.shape, BF16), grad, grad, grad),
        in_specs=[anyw] * 2,
        out_specs=(pl.BlockSpec(memory_space=pltpu.HBM),) * 4,
        scratch_shapes=[pltpu.SemaphoreType.DMA((10,))],
        compiler_params=pltpu.CompilerParams(vmem_limit_bytes=1024 * 1024),
    )(hidden, sums)


def on_device(tokens, out_grad, counts, block_moves, segment_ids, gate, up, down):
    seg = segment_ids.reshape(CAP, BLOCK)
    hidden, sums = big(counts, block_moves.T, seg, tokens, out_grad, gate, up, down)
    return finish(hidden, sums)


def solution(mesh):
    torus = Mesh(mesh.devices.reshape(NY, NX, NZ, 2), ("y", "x", "z", "core"))
    row, col = ("y", "x"), ("z", "core")
    return jax.shard_map(
        on_device,
        mesh=torus,
        in_specs=(P(row, col), P(row, col), P(row), P(), P(row), P(row, col), P(row, col), P(row, col)),
        out_specs=(P(row, col),) * 4,
        check_vma=False,
    )
```

```python
import random

import jax
import jax.numpy as jnp
from jax import lax
from jax.experimental import pallas as pl
from jax.experimental.pallas import tpu as pltpu
from jax.sharding import Mesh
from jax.sharding import PartitionSpec as P

BLOCK = 128
WORK = 4
CAP = 6
MOVES = 16
NX, NY, NZ = 4, 8, 8
ROWS = 64
HID = 512
PART = HID // 2
COLS = 3 * PART
RANK = WORK * BLOCK
MAIN = 384
MSG = 2 * BLOCK + 16
YMSG = BLOCK + 16
CUT = {"a": (0, 384), "b": (384, 384)}
LOAD = {"a": (0, 512), "b": (512, 256)}
LINKS = ("x+", "x-", "y+", "y-", "z+", "z-", "core", "pair")
PAIRED = (2, 3)
RING = 4
MESH = pl.DeviceIdType.MESH
BF16, F32 = jnp.bfloat16, jnp.float32


def factor(flag):
    return jnp.where(flag, 1.0, 0.0).astype(F32)


def choose(me, count, moves):
    zero, one = jnp.int32(0), jnp.int32(1)
    left = zero
    leaving = [-one] * 2
    arrives = zero
    for m in range(MOVES):
        mine = moves[0, m] == me
        for j in range(2):
            leaving[j] = jnp.where(mine & (left == j), moves[2, m], leaving[j])
        left = left + jnp.where(mine, one, zero)
        arrives = arrives | jnp.where(moves[1, m] == me, one, zero)
    kept = zero
    chosen = [-one] * WORK
    for b in range(CAP):
        stays = (b * BLOCK < count) & (leaving[0] != b) & (leaving[1] != b)
        for s in range(WORK):
            chosen[s] = jnp.where(stays & (kept == s), jnp.int32(b), chosen[s])
        kept = kept + jnp.where(stays, one, zero)
    stay = [[factor(chosen[s] == b) for b in range(CAP)] for s in range(WORK)]
    leave = [[factor(leaving[j] == b) for b in range(CAP)] for j in range(2)]
    slot = [factor((arrives == 1) & (kept == s)) for s in range(WORK)]
    return stay, leave, slot


def routes(y, x, moves):
    zero, one = jnp.int32(0), jnp.int32(1)
    src = [moves[0, m] for m in range(MOVES)]
    dst = [moves[1, m] for m in range(MOVES)]
    number = []
    for m in range(MOVES):
        second = zero
        for before in range(m):
            second = second | jnp.where(src[before] == src[m], one, zero)
        here = (src[m] >= y * NX) & (src[m] < y * NX + NX)
        number.append(jnp.where(here, (src[m] - y * NX) * 2 + second, -one))
    result = []
    for d in range(NY):
        at = -one
        for m in range(MOVES):
            at = jnp.where(dst[m] == d * NX + x, number[m], at)
        result.append([factor(at == i) for i in range(2 * NX)])
    return result


def blend(factors, blocks):
    total = None
    for f, block in zip(factors, blocks):
        term = block * f.astype(BF16)
        total = term if total is None else total + term
    return total


class Graph:
    def __init__(self):
        self.nodes = {}

    def send(self, name, link, size, needs, make, silent):
        self.nodes[name] = ("send", link, size, tuple(needs), make, silent)

    def work(self, name, cost, rank, needs, run):
        self.nodes[name] = ("work", cost, rank, tuple(needs), run)

    rate, lag = 46.6e3, 2.5
    early, late, along_z = 0.8, 1.0, 1.0
    seed, noise = 0, 0.0

    def span(self, n):
        node = self.nodes[n]
        if node[0] == "work":
            return node[1]
        quick = node[1] == "core"
        return node[2] / (self.rate * (12 if quick else 1)) + (1.0 if quick else self.lag)

    def order(self):
        nodes = self.nodes
        after = {n: [] for n in nodes}
        for n, node in nodes.items():
            for m in node[3]:
                after[m].append(n)
        below = {}

        def urgency(n):
            if n not in below:
                below[n] = self.span(n) + max([urgency(m) for m in after[n]], default=0.0)
            return below[n]

        draw = random.Random(self.seed)
        moved = {n: urgency(n) + draw.uniform(0.0, self.noise) for n in nodes}
        todo = sorted(nodes, key=lambda n: -moved[n])
        done, flying, free, now, steps, times = set(), [], {}, 0.0, [], {}
        while todo or flying:
            landed = ("pl", 1) in done
            for name in [n for n in todo if nodes[n][0] == "send"]:
                _, link, size, needs = nodes[name][:4]
                ways = ("x+", "x-") if link == "pair" else (link,)
                ahead = self.along_z if link in ("z+", "z-", "core") else self.late if landed else self.early
                begin = max([now] + [free.get(way, 0.0) for way in ways])
                if all(n in done for n in needs) and begin - now < ahead:
                    quick = link == "core"
                    ends = begin + size / (self.rate * (12 if quick else 1))
                    for way in ways:
                        free[way] = ends
                    flying.append((ends + (1.0 if quick else self.lag), len(steps), name))
                    steps.append(("start", name))
                    todo.remove(name)
            flying.sort()
            if flying and flying[0][0] <= now:
                name = flying.pop(0)[2]
                if not nodes[name][5]:
                    steps.append(("wait", name))
                times[name] = now
                done.add(name)
                continue
            ready = [n for n in todo if nodes[n][0] == "work" and all(m in done for m in nodes[n][3])]
            if ready:
                steps.append(("run", ready[0]))
                now += nodes[ready[0]][1]
                times[ready[0]] = now
                done.add(ready[0])
                todo.remove(ready[0])
                continue
            if flying:
                now = flying[0][0]
        times["end"] = now
        self.times = times
        return steps


def big_kernel(counts_hbm, moves_hbm, seg_hbm, tok, grad, gate, up, down, hidden, sums_out,
               w, z, xt, acc, act, tb, tb2, slots_a, slots_o, slots_s, slots_y, slots_m, xbuf, ysend, own3, tokv, gradv,
               marks, hbuf, counts, moves, seg, send_sem, recv_sem, own_sem):
    y, x = lax.axis_index("y"), lax.axis_index("x")
    zz, core = lax.axis_index("z"), lax.axis_index("core")
    size_of = {"x": NX, "y": NY, "z": NZ}
    mine = {"x": x, "y": y, "z": zz}
    side = lax.rem(x, 2)
    pair = x + 1 - 2 * side

    def step(axis, by):
        return lax.rem(mine[axis] + (by % size_of[axis]), size_of[axis])

    barrier = pltpu.get_barrier_semaphore()
    peers = [{axis: step(axis, by)} for axis in ("x", "y", "z") for by in (1, -1)] + [{"core": 1 - core}]
    for peer in peers:
        pl.semaphore_signal(barrier, inc=1, device_id=peer, device_id_type=MESH)

    own_rows = pl.ds(pl.multiple_of((y * NX + x) * ROWS, ROWS), ROWS)
    feature = zz * 2 + core
    local_rows = [
        pltpu.make_async_copy(tok, tokv, own_sem.at[0]),
        pltpu.make_async_copy(grad, gradv, own_sem.at[1]),
    ]
    local = [
        pltpu.make_async_copy(
            ref.at[:, pl.ds(p * PART, PART)], w.at[p, own_rows, pl.ds(i * PART, PART)], own_sem.at[2 + 2 * i + p]
        )
        for i, ref in enumerate((gate, up, down))
        for p in range(2)
    ]
    small = [
        pltpu.make_async_copy(ref, held, own_sem.at[8 + i])
        for i, (ref, held) in enumerate(((counts_hbm, counts), (moves_hbm, moves), (seg_hbm, seg)))
    ]
    for copy in small + local_rows + local:
        copy.start()
    for copy in small:
        copy.wait()
    stay, leave, slot_of = choose(y * NX + x, counts[0], moves)
    route = []

    graph = Graph()
    index = {}

    def remote(name, link, size, needs, peer, views, shared=None):
        i = index.setdefault(shared or name, len(index))

        def make(receiver, at=0):
            source, target = views(receiver)
            return pltpu.make_async_remote_copy(
                src_ref=source, dst_ref=target, send_sem=send_sem.at[at], recv_sem=recv_sem.at[i],
                device_id=peer, device_id_type=MESH,
            )

        graph.send(name, link, size, needs, make, shared is not None)

    def join(shared, members, ref):
        def wait():
            pltpu.make_async_copy(ref(), ref(), recv_sem.at[index[shared]]).wait()

        graph.work(shared, 0.0, 0, members, wait)

    def spread(tag, axis, size, needs, piece, hops=None):
        n = size_of[axis]
        arrived = {0: list(needs)}
        far = (tag, "far")
        hops = n // 2 if hops is None else hops
        for hop in range(1, hops + 1):
            base = hop - 1
            for sign in (1, -1):
                part = None if hop < n // 2 else (0 if sign > 0 else 1)

                def views(receiver, sign=sign, hop=hop, base=base, part=part):
                    ref = piece(step(axis, -sign * (hop if receiver else base)), part)
                    return ref, ref

                share = size if part is None else size // 2
                remote((tag, sign, hop), axis + "-+"[sign > 0], share * (hop - base),
                       [(tag, sign, base)] if base else needs, {axis: step(axis, sign * (hop - base))}, views,
                       None if part is None else far)
                if part is None:
                    arrived[sign * hop % n] = [(tag, sign, hop)]
        if hops == n // 2:
            join(far, [(tag, 1, n // 2), (tag, -1, n // 2)], lambda: piece(step(axis, n // 2), None))
            arrived[n // 2] = [far]
        return arrived

    def x_spread(tag, size, needs, other_needs, piece, forwarded):
        far = (tag, "far")
        for sign in (1, -1):
            part = 0 if sign > 0 else 1
            for hop in (1, 2):
                def same(receiver, sign=sign, hop=hop, part=part):
                    origin = step("x", -sign * (hop if receiver else hop - 1))
                    ref = piece(origin, lax.rem(origin, 2), part)
                    return ref, ref

                remote((tag, sign, hop), "x" + "-+"[sign > 0], size // 2, needs if hop == 1 else [(tag, sign, 1)],
                       {"x": step("x", sign)}, same, None if hop == 1 else far)

            def other(receiver, sign=sign):
                origin = step("x", -sign if receiver else 0)
                ref = piece(origin, 1 - lax.rem(origin, 2), None)
                return ref, ref

            remote((tag, sign, 0), "x" + "-+"[sign > 0], size, other_needs, {"x": step("x", sign)}, other,
                   None if forwarded else far)
        if forwarded:
            join(far, [(tag, 1, 2), (tag, -1, 2)], lambda: w.at[0, pl.ds(0, ROWS), pl.ds(*LOAD["a"])])
            return {0: list(needs), 1: [(tag, 1, 0)], 3: [(tag, -1, 0)], 2: [far]}
        join(far, [(tag, sign, hop) for sign in (1, -1) for hop in (0, 2)],
             lambda: w.at[0, pl.ds(0, 3 * ROWS), pl.ds(*LOAD["b"])])
        return {0: list(needs), 1: [far], 3: [far], 2: [far]}

    def gather_sum(tag, axis, size, own_ready, piece, cost, finish, pool, halves):
        n = size_of[axis]
        slot = {}
        slots, used = pool
        near = (tag, "near")
        for hop in range(n // 2, 0, -1):
            for sign in (1, -1):
                name = (tag, sign, hop)
                part = None if hop < n // 2 else (0 if sign > 0 else 1)
                slot[sign, hop] = ref = slots.at[len(used)]
                used.append(name)
                if part is not None:
                    ref = halves(ref, part)

                def views(receiver, sign=sign, hop=hop, part=part, ref=ref):
                    return piece(step(axis, sign * hop), part), ref

                needs = own_ready(sign * hop % n) if hop == n // 2 else [("add", tag, sign, hop)]
                remote(name, axis + "-+"[sign > 0], size if part is None else size // 2, needs,
                       {axis: step(axis, sign)}, views, None if hop > 1 else near)
                if hop > 1:

                    def add(sign=sign, hop=hop, part=part, ref=ref):
                        into = piece(step(axis, sign * (hop - 1)), part)
                        into[...] = (into[...].astype(F32) + ref[...].astype(F32)).astype(BF16)

                    graph.work(("add", tag, sign, hop - 1), cost, 0,
                               [name] + own_ready(sign * (hop - 1) % n), add)

        def fin():
            finish(piece(mine[axis], None), slot[1, 1], slot[-1, 1])

        join(near, [(tag, 1, 1), (tag, -1, 1)], lambda: slots.at[pl.ds(0, 2)])
        graph.work(("fin", tag), 1.5 * cost, 0, [near] + own_ready(0), fin)

    def x_sum(tag, size, own_ready, piece, finish, at):
        near = (tag, "near")
        for sign in (1, -1):
            part = 0 if sign > 0 else 1
            way, peer = "x" + "-+"[sign > 0], {"x": step("x", sign)}
            first, second = slots_s.at[at, 2 * part], slots_s.at[at, 2 * part + 1]
            remote((tag, sign, 2), way, size // 2, own_ready(2), peer,
                   lambda r, part=part, first=first: (piece(step("x", 2), part), first))
            remote((tag, sign, 1), way, size // 2, [(tag, sign, 2)], peer,
                   lambda r, first=first, second=second: (first, second), near)
            remote((tag, sign, 0), way, size, own_ready(sign % NX), peer,
                   lambda r, sign=sign, part=part: (piece(step("x", sign), None), slots_o.at[at, part]), near)

        def fin():
            own_ref = piece(x, None)
            own = own_ref[...].astype(F32)
            two_on = jnp.concatenate([slots_s[at, 1], slots_s[at, 3]], axis=0).astype(F32)
            finish(own + two_on, slots_o[at, 0].astype(F32) + slots_o[at, 1].astype(F32))

        join(near, [(tag, s, h) for s in (1, -1) for h in (1, 0)], lambda: slots_a.at[pl.ds(0, 3)])
        graph.work(("fin", tag), 0.15, 0, [near] + own_ready(0), fin)

    pool_a, pool_y, pool_m = (slots_a, []), (slots_y, []), (slots_m, [])

    def prepare():
        lane = lax.broadcasted_iota(jnp.int32, (8, BLOCK), 1)
        line = lax.broadcasted_iota(jnp.int32, (8, BLOCK), 0)
        now = jnp.concatenate([seg[...], seg[0:2, :]], axis=0)
        down_one = jnp.concatenate([now[1:8, :], now[0:1, :]], axis=0)
        after = jnp.where(lane == BLOCK - 1, down_one[:, 0:1], pltpu.roll(now, BLOCK - 1, 1))
        keep = jnp.where((line * BLOCK + lane + 1 < counts[0]) & (after == now), 1.0, 0.0).astype(F32)
        marks[...] = jnp.zeros_like(marks)
        marks[pl.ds(0, 8), :] = keep
        columns = marks[...].T
        for copy in local_rows:
            copy.wait()
        for b in range(CAP):
            at = pl.ds(b * BLOCK, BLOCK)
            gradv[at, :] = (gradv[at, :].astype(F32) * columns[:, b : b + 1]).astype(BF16)
        blocks = [pl.ds(b * BLOCK, BLOCK) for b in range(CAP)]
        for t, ref in enumerate((tokv, gradv)):
            for j in range(2):
                xbuf[t, x, pl.ds(j * BLOCK, BLOCK), :] = blend(leave[j], [ref[at, :] for at in blocks])
        total = jnp.sum(jnp.sum(keep, axis=0, keepdims=True), axis=1, keepdims=True)
        high = jnp.floor(total * (1 / 256))
        middle = jnp.floor((total - 256.0 * high) * (1 / 16))
        low = total - 256.0 * high - 16.0 * middle
        row = lax.broadcasted_iota(jnp.int32, (16, BLOCK), 0) - 3 * x
        digits = jnp.where(row == 0, high, jnp.where(row == 1, middle, jnp.where(row == 2, low, 0.0)))
        for t in range(2):
            xbuf[t, x, pl.ds(2 * BLOCK, 16), :] = digits.astype(BF16)

    def rank_rows(of, lo, n):
        return pl.ds(pl.multiple_of(of * RANK + lo, BLOCK), n)

    def prepare_own():
        blocks = [pl.ds(b * BLOCK, BLOCK) for b in range(CAP)]
        for t, ref in enumerate((tokv, gradv)):
            for s in range(WORK):
                rows = blend(stay[s][s:], [ref[at, :] for at in blocks[s:]])
                if s < WORK - 1:
                    z[feature, t, rank_rows(side, s * BLOCK, BLOCK), :] = rows
                else:
                    own3[t] = rows

    graph.work("own", 0.3, 0, [], prepare_own)

    graph.work("route", 0.5, 0, [], lambda: route.extend(routes(y, x, moves)))
    mx = []
    for t in range(2):
        def message(o, part, t=t):
            lo, n = (0, MSG) if part is None else ((0, BLOCK), (BLOCK, MSG - BLOCK))[part]
            return xbuf.at[t, o, pl.ds(lo, n), :]

        mx.append(spread(("mx", t), "x", MSG * BLOCK * 2, [], message))
    mx_first = mx[0][1] + mx[0][3] + mx[1][1] + mx[1][3]

    def select(t):
        digits = sum(xbuf[t, i, pl.ds(2 * BLOCK, 16), :].astype(F32) for i in range(NX)).astype(BF16)
        blocks = [xbuf[t, i // 2, pl.ds(i % 2 * BLOCK, BLOCK), :] for i in range(2 * NX)]
        for d in range(NY):
            ysend[t, d, pl.ds(0, BLOCK), :] = blend(route[d], blocks)
            ysend[t, d, pl.ds(BLOCK, 16), :] = digits

    move_halves = (pl.ds(0, BLOCK // 2), pl.ds(BLOCK // 2, YMSG - BLOCK // 2))
    cut_move = lambda ref, part: ref.at[move_halves[part], :]
    for t in range(2):
        graph.work(("select", t), 0.3, 0, ["route"] + [n for names in mx[t].values() for n in names], lambda t=t: select(t))

        def merge(own_ref, one, other, t=t):
            total = own_ref[...].astype(F32) + one[...].astype(F32) + other[...].astype(F32)
            z[feature, t, rank_rows(side, MAIN, BLOCK), :] = (total[0:BLOCK] + own3[t].astype(F32)).astype(BF16)
            own_ref[...] = total.astype(BF16)

        gather_sum(("my", t), "y", YMSG * BLOCK * 2, lambda j, t=t: [("select", t)] + ([] if j else ["own"]),
                   lambda o, part, t=t: ysend.at[t, o] if part is None else ysend.at[t, o, move_halves[part], :],
                   0.1, merge, pool_m, cut_move)

        def handed(receiver, t=t):
            ref = z.at[feature, t, rank_rows(1 - side if receiver else side, MAIN, BLOCK), :]
            return ref, ref

        remote(("pl", t), "pair", BLOCK * BLOCK * 2, [("fin", ("my", t))], {"x": pair}, handed)

    def loss_total():
        digits = ysend[0, y, pl.ds(BLOCK, 16), :].astype(F32)
        row = lax.broadcasted_iota(jnp.int32, (16, BLOCK), 0) % 3
        parts = jnp.where(row == 0, 256.0 * digits, jnp.where(row == 1, 16.0 * digits, digits))
        return jnp.sum(parts, axis=0, keepdims=True)[:, 0:1]

    def shard_rows(at_y, at_x, part):
        first = pl.multiple_of((at_y * NX + at_x) * ROWS + (32 if part else 0), 32)
        return pl.ds(first, ROWS if part is None else 32)

    def shard(of, at_y, at_x, cut, part):
        return w.at[of, shard_rows(at_y, at_x, part), pl.ds(*LOAD[cut])]

    load_a, load_b = (ROWS * LOAD[cut][1] * 2 for cut in "ab")
    by_own = spread("by", "y", load_b, [], lambda o, part: shard(side, o, x, "b", part))
    by_other = spread("bz", "y", load_b, [], lambda o, part: shard(1 - side, o, x, "b", part))
    ax = x_spread("ax", load_a, mx_first, mx_first, lambda o, of, part: shard(of, y, o, "a", part), True)
    ay, bx = {}, {}
    for e in ax:
        ay[e] = spread(("ay", e), "y", load_a, ax[e], lambda o, part, e=e: shard(side, o, step("x", -e), "a", part))
    for f in by_own:
        bx[f] = x_spread(("bx", f), load_b, by_own[f] or mx_first, by_other[f] or mx_first,
                         lambda o, of, part, f=f: shard(of, step("y", -f), o, "b", part), False)

    def hand(name, lo, n, needs):
        def views(receiver):
            ref = z.at[feature, :, rank_rows(1 - side if receiver else side, lo, n), :]
            return ref, ref

        remote(name, "pair", 2 * n * BLOCK * 2, needs, {"x": pair}, views)

    hand("pm", 0, MAIN, ["own"] + mx_first)
    have, turns, landed_of = {}, [], {}

    def turn(c, t, of, lo, n_rows):
        rows = rank_rows(of, lo, n_rows)
        xt[t, pl.ds(pl.multiple_of(c * BLOCK, BLOCK), BLOCK), rows] = z[c, t, rows, :].T

    for tag, of, lo, rows, needs in (
        ("zm", side, 0, MAIN, ["own"]), ("zp", 1 - side, 0, MAIN, ["pm"]),
        ("zl", side, MAIN, BLOCK, []), ("zq", 1 - side, MAIN, BLOCK, []),
    ):
        have[tag] = []
        for t in range(2):
            def cut(at, part, of=of, lo=lo, rows=rows, t=t):
                if part is None:
                    return z.at[at, t, rank_rows(of, lo, rows), :]
                first = pl.multiple_of(of * RANK + lo + part * (rows // 2), 64)
                return z.at[at, t, pl.ds(first, rows // 2), :]

            size = rows * BLOCK * 2
            begin = {"zl": [("fin", ("my", t))], "zq": [("pl", t)]}.get(tag, needs)
            hops = PAIRED[t] if tag == "zp" else NZ // 2
            arrived = spread((tag, t), "z", size, begin, lambda o, part, cut=cut: cut(o * 2 + core, part), hops)
            landed_of[tag, t] = arrived
            for g in range(hops + 1, NZ - hops):

                def views(receiver, t=t, g=g):
                    ref = z.at[step("z", -g) * 2 + core, t, rank_rows(1 - side if receiver else side, 0, MAIN), :]
                    return ref, ref

                remote((tag, t, g), "pair", size, landed_of["zm", t][g], {"x": pair}, views)
                arrived[g] = [(tag, t, g)]
            shared = ("core", tag, t)
            for g, names in arrived.items():
                def views(receiver, g=g, cut=cut):
                    ref = cut(step("z", -g) * 2 + (1 - core if receiver else core), None)
                    return ref, ref

                remote((shared, g), "core", size, names, {"core": 1 - core}, views, shared)
            join(shared, [(shared, g) for g in arrived],
                 lambda of=of, lo=lo, rows=rows, t=t: z.at[pl.ds(0, NZ), t, rank_rows(of, lo, rows), :])
            have[tag] += [shared] + [name for names in arrived.values() for name in names]
            for g, names in arrived.items():
                for far in range(2):
                    turns.append(("turn", tag, t, g, far))
                    graph.work(turns[-1], 0.1 if lo == 0 else 0.04, 3, [shared] if far else names,
                               lambda g=g, far=far, t=t, of=of, lo=lo, rows=rows: turn(
                                   step("z", -g) * 2 + (1 - core if far else core), t, of, lo, rows))

    seen = []

    def forward(f, tag, of):
        start = tag not in seen
        seen.append(tag)
        at = step("y", -f)
        rows = pl.ds(pl.multiple_of(at * 256, 256), 256)
        slots = rank_rows(of, 0, MAIN)
        for t, lo, n in ((0, 0, 2 * PART), (1, 2 * PART, PART)):
            left = jnp.concatenate([z[at * 2, t, slots, :], z[at * 2 + 1, t, slots, :]], axis=1)
            cols = pl.ds(lo, n)
            new = jnp.dot(left, w[side, rows, cols], preferred_element_type=F32)
            acc[slots, cols] = new if start else acc[slots, cols] + new

    def forward_last(of):
        slots = rank_rows(of, MAIN, BLOCK)
        for t, lo, n in ((0, 0, 2 * PART), (1, 2 * PART, PART)):
            left = jnp.concatenate([z[c, t, slots, :] for c in range(2 * NZ)], axis=1)
            cols = pl.ds(lo, n)
            acc[slots, cols] = jnp.dot(left, w[side, :, cols], preferred_element_type=F32)

    all_landed = []
    for f in range(NY):
        landed = [n for e in ay for n in ay[e][f]] + [n for e in bx[f] for n in bx[f][e]]
        all_landed += landed
        for tag, of in (("zm", side), ("zp", 1 - side)):
            graph.work(("fwd", tag, f), 0.6, 2, have[tag] + landed, lambda f=f, tag=tag, of=of: forward(f, tag, of))
    for tag, of in (("zl", side), ("zq", 1 - side)):
        graph.work(("fwd last", tag), 0.8, 2, have[tag] + all_landed, lambda of=of: forward_last(of))

    def pointwise(of, lo, n):
        def rows_of(i, _):
            rows = pl.ds(pl.multiple_of(of * RANK + lo + i * 64, 64), 64)
            g, u, b = acc[rows, 0:PART], acc[rows, PART : 2 * PART], acc[rows, 2 * PART : COLS]
            logistic = jax.nn.sigmoid(g)
            activated = g * logistic
            act[rows, 0:PART] = (b * u * logistic * (1.0 + g * (1.0 - logistic))).astype(BF16)
            act[rows, PART : 2 * PART] = (b * activated).astype(BF16)
            act[rows, 2 * PART : COLS] = (activated * u).astype(BF16)
            return 0

        lax.fori_loop(0, n // 64, rows_of, 0)

    for tag, of in (("zm", side), ("zp", 1 - side)):
        graph.work(("pointwise", tag), 0.25, 2, [("fwd", tag, f) for f in range(NY)], lambda of=of: pointwise(of, 0, MAIN))
    for tag, of in (("zl", side), ("zq", 1 - side)):
        graph.work(("pointwise", tag), 0.1, 2, [("fwd last", tag)], lambda of=of: pointwise(of, MAIN, BLOCK))
    graph.work("pointwise", 0.0, 2, [("pointwise", tag) for tag in have] + turns, lambda: None)

    for i in range(WORK):
        def views(receiver, i=i):
            here = act.at[rank_rows(1 - side, i * BLOCK, BLOCK), pl.ds(2 * PART, PART)]
            return here, hbuf.at[pl.ds(i * BLOCK, BLOCK), :]

        remote(("hidden", i), "pair", BLOCK * PART * 2, [("bwd", 0)] if i else ["pointwise"], {"x": pair}, views)

    def store_hidden():
        stays = 1.0 - (slot_of[0] + slot_of[1] + slot_of[2])
        for which in range(2):
            cols = pl.ds(pl.multiple_of((side if which == 0 else 1 - side) * PART, PART), PART)

            def rows(s, which=which):
                if which == 0:
                    return act[rank_rows(side, s * BLOCK, BLOCK), 2 * PART : COLS]
                return hbuf[pl.ds(s * BLOCK, BLOCK), :]

            last = rows(WORK - 1)
            for s in range(WORK - 1):
                hidden[pl.ds(s * BLOCK, BLOCK), cols] = rows(s) + last * slot_of[s].astype(BF16)
            hidden[pl.ds(MAIN, BLOCK), cols] = last * stays.astype(BF16)

    graph.work("store hidden", 0.3, 9, [("hidden", i) for i in range(WORK)], store_hidden)

    def backward(j, spans):
        rows = pl.ds(pl.multiple_of(step("y", j) * 256, 256), 256)
        for t, lo, n in spans:
            cols = pl.ds(lo, n)
            tb[rows, cols] = jnp.dot(xt[t, rows, :], act[:, cols], preferred_element_type=F32).astype(BF16)

    first_b, edge = CUT["b"][0], 2 * PART
    graph.work(("bwd", 4, "b"), 0.45, 0, ["pointwise"],
               lambda: backward(4, ((0, first_b, edge - first_b), (1, edge, COLS - edge))))
    graph.work(("bwd", 4, "a"), 0.4, 0, ["pointwise", ("bwd", 4, "b")], lambda: backward(4, ((0, 0, first_b),)))
    for i, j in enumerate((5, 3, 6, 2, 7, 1, 0)):
        graph.work(("bwd", j), 0.8, 1 + i, ["pointwise"], lambda j=j: backward(j, ((0, 0, edge), (1, edge, PART))))

    def done_of(j, cut):
        return [("bwd", j, cut)] if j == 4 else [("bwd", j)]

    size_a, size_b = (ROWS * CUT[cut][1] * 2 for cut in "ab")

    def plain(own_ref, one, other):
        own_ref[...] = (own_ref[...].astype(F32) + one[...].astype(F32) + other[...].astype(F32)).astype(BF16)

    def final_a(same, other):
        total = loss_total()
        sums_out[side, :, pl.ds(*CUT["a"])] = same / total
        sums_out[1 - side, :, pl.ds(*CUT["a"])] = other / total

    def final_b(p):
        def run(own_ref, one, other):
            sums = own_ref[...].astype(F32) + one[...].astype(F32) + other[...].astype(F32)
            sums_out[p, :, pl.ds(*CUT["b"])] = sums / loss_total()
        return run

    def term(at_y, at_x, cut, part):
        return tb.at[shard_rows(at_y, at_x, part), pl.ds(*CUT[cut])]

    row_halves = (pl.ds(0, 32), pl.ds(32, 32))
    for e in (2, 1, 3, 0):
        gather_sum(("say", e), "y", size_a, lambda j: done_of(j, "a"),
                   lambda o, part, e=e: term(o, step("x", e), "a", part), 0.1, plain, pool_a,
                   lambda ref, part: ref.at[row_halves[part], :])
    for f in (4, 5, 3, 6, 2, 7, 1, 0):
        def keep(same, other, f=f):
            at = step("y", f)
            tb2[at, side] = same.astype(BF16)
            tb2[at, 1 - side] = other.astype(BF16)

        x_sum(("sbx", f), size_b, lambda e, f=f: done_of(f, "b"),
              lambda o, part, f=f: term(step("y", f), o, "b", part), keep, f)
    x_sum("sax", size_a, lambda e: [("fin", ("say", e))], lambda o, part: term(y, o, "a", part), final_a, NY)

    for p in range(2):
        gather_sum(("sby", p), "y", size_b, lambda j: [("fin", ("sbx", j))],
                   lambda o, part, p=p: tb2.at[o, p] if part is None else tb2.at[o, p, row_halves[part], :], 0.1,
                   final_b(p), pool_y, lambda ref, part: ref.at[row_halves[part], :])

    prepare()
    for copy in local:
        copy.wait()
    pl.semaphore_wait(barrier, len(peers))
    started = {link: [] for link in LINKS}
    for kind, name in graph.order():
        node = graph.nodes[name]
        if kind == "run":
            node[4]()
        elif kind == "start":
            mates = started[node[1]]
            if len(mates) >= RING:
                mates[-RING].wait_send()
            copy = node[4](False, LINKS.index(node[1]) * RING + len(mates) % RING)
            copy.start()
            mates.append(copy)
        else:
            node[4](True).wait_recv()
    for mates in started.values():
        for copy in mates[-RING:]:
            copy.wait_send()
    assert len(index) == RECEIVES


RECEIVES = 231


def big(counts, moves, seg, tok, grad, gate, up, down):
    anyw, hbm = pl.BlockSpec(memory_space=pl.ANY), pl.BlockSpec(memory_space=pltpu.HBM)
    width = NX * NY * ROWS
    wide_a, wide_b = CUT["a"][1], CUT["b"][1]
    return pl.pallas_call(
        big_kernel,
        out_shape=(pltpu.VMEM((RANK, HID), BF16), pltpu.VMEM((2, ROWS, COLS), F32)),
        in_specs=[hbm] * 8,
        out_specs=(pl.BlockSpec(memory_space=pltpu.VMEM),) * 2,
        scratch_shapes=[
            pltpu.VMEM((2, width, COLS), BF16),
            pltpu.VMEM((2 * NZ, 2, 2 * RANK, BLOCK), BF16),
            pltpu.VMEM((2, width, 2 * RANK), BF16),
            pltpu.VMEM((2 * RANK, COLS), F32),
            pltpu.VMEM((2 * RANK, COLS), BF16),
            pltpu.VMEM((width, COLS), BF16),
            pltpu.VMEM((NY, 2, ROWS, wide_b), BF16),
            pltpu.VMEM((32, ROWS, wide_a), BF16),
            pltpu.VMEM((NY + 1, 2, ROWS, wide_b), BF16),
            pltpu.VMEM((NY + 1, 4, ROWS // 2, wide_b), BF16),
            pltpu.VMEM((16, ROWS, wide_b), BF16),
            pltpu.VMEM((16, YMSG, BLOCK), BF16),
            pltpu.VMEM((2, NX, MSG, BLOCK), BF16),
            pltpu.VMEM((2, NY, YMSG, BLOCK), BF16),
            pltpu.VMEM((2, BLOCK, BLOCK), BF16),
            pltpu.VMEM((CAP * BLOCK, BLOCK), BF16),
            pltpu.VMEM((CAP * BLOCK, BLOCK), BF16),
            pltpu.VMEM((BLOCK, BLOCK), F32),
            pltpu.VMEM((RANK, PART), BF16),
            pltpu.SMEM((1,), jnp.int32),
            pltpu.SMEM((3, MOVES), jnp.int32),
            pltpu.VMEM((CAP, BLOCK), jnp.int32),
            pltpu.SemaphoreType.DMA((RING * len(LINKS),)),
            pltpu.SemaphoreType.DMA((RECEIVES,)),
            pltpu.SemaphoreType.DMA((11,)),
        ],
        compiler_params=pltpu.CompilerParams(
            collective_id=0, has_side_effects=True, vmem_limit_bytes=60 * 1024 * 1024
        ),
    )(counts, moves, seg, tok, grad, gate, up, down)


def finish_kernel(hidden_in, sums, hidden, gate_out, up_out, down_out, sems):
    quarter = RANK // 4
    copies = [
        pltpu.make_async_copy(hidden_in.at[pl.ds(i * quarter, quarter), :], hidden.at[pl.ds(i * quarter, quarter), :], sems.at[i])
        for i in range(4)
    ]
    copies += [
        pltpu.make_async_copy(sums.at[p, :, pl.ds(i * PART, PART)], out.at[:, pl.ds(p * PART, PART)], sems.at[4 + 2 * i + p])
        for i, out in enumerate((gate_out, up_out, down_out))
        for p in range(2)
    ]
    for copy in copies:
        copy.start()
    for copy in copies:
        copy.wait()


def finish(hidden, sums):
    anyw = pl.BlockSpec(memory_space=pl.ANY)
    grad = jax.ShapeDtypeStruct((ROWS, HID), F32)
    return pl.pallas_call(
        finish_kernel,
        out_shape=(jax.ShapeDtypeStruct(hidden.shape, BF16), grad, grad, grad),
        in_specs=[anyw] * 2,
        out_specs=(pl.BlockSpec(memory_space=pltpu.HBM),) * 4,
        scratch_shapes=[pltpu.SemaphoreType.DMA((10,))],
        compiler_params=pltpu.CompilerParams(vmem_limit_bytes=1024 * 1024),
    )(hidden, sums)


def on_device(tokens, out_grad, counts, block_moves, segment_ids, gate, up, down):
    seg = segment_ids.reshape(CAP, BLOCK)
    hidden, sums = big(counts, block_moves.T, seg, tokens, out_grad, gate, up, down)
    return finish(hidden, sums)


def solution(mesh):
    torus = Mesh(mesh.devices.reshape(NY, NX, NZ, 2), ("y", "x", "z", "core"))
    row, col = ("y", "x"), ("z", "core")
    return jax.shard_map(
        on_device,
        mesh=torus,
        in_specs=(P(row, col), P(row, col), P(row), P(), P(row), P(row, col), P(row, col), P(row, col)),
        out_specs=(P(row, col),) * 4,
        check_vma=False,
    )
```
